256 devices in a mesh: row: 8 (over z), col: 32 (over x, y, core).
Axes of the slice: x: 4, y: 4, z: 8, core: 2. Of those that a mesh axis runs over, the one named last changes fastest.
Arguments:
- rhs: float32 [64, 131072], P(None, ('row', 'col')), may hold values from -6 to 6
- pivots: int32 [4096], replicated, may hold values from 0 to 131071, as said below
- factor: float32 [4096, 1, 32, 128], P('row', None, 'col'), as said below
- diag_inv: float32 [8, 512, 512], P('row'), as said below
Outputs:
- solution: float32 [64, 1, 32, 128], P(None, None, 'col')
The draws below stay inside these ranges and needn't reach their ends.
Inputs may be any that keep to these rules, and one draw needn't show every extreme that they name: `pivots`: distinct column numbers, the first 4096 entries of a permutation of 0 .. 131071. `factor`: entry (row i, column q) is zero where q >= 512 * (i // 512). `diag_inv`: each block is unit lower triangular.
All inputs are finite; a program needn't handle non-finite values.
Results may differ from the reference program's by a relative error of at most 0.0001.
Values sent between devices are 32-bit elements; how exact they have to be, the bound alone decides.
No kernel may reach another device: no remote copies, remote signals or barrier semaphores. Data moves between devices by JAX's collectives and lax.ppermute only.
A program may use at most 64 MiB of HBM per device.

```python
import math
import jax
import jax.numpy as jnp
from jax import lax

N = 131072
BLK = 512
CB = 128
NRHS = 64
NB = 8
N_COL = 32


def draw_pivots(key, part):
    order = jax.random.permutation(jax.random.fold_in(key, 11), N)
    return order[:NB * BLK].astype(jnp.int32)


def draw_factor(key, part):
    width = NB * BLK
    rounds = NB * (BLK // CB) // N_COL
    shape = (width, rounds, N_COL, CB)
    row_block = lax.broadcasted_iota(jnp.int32, shape, 0) // BLK
    column = (lax.broadcasted_iota(jnp.int32, shape, 1) * N_COL + lax.broadcasted_iota(jnp.int32, shape, 2)) * CB + lax.broadcasted_iota(jnp.int32, shape, 3)
    col_block = column // BLK
    subkey = jax.random.fold_in(key, 23)
    values = jax.random.normal(subkey, shape, jnp.float32)
    values = values * (0.6 / math.sqrt(width))
    return jnp.where(col_block < row_block, values, 0.0).astype(jnp.float32)


def draw_diag_inv(key, part):
    shape = (NB, BLK, BLK)
    inner = lax.broadcasted_iota(jnp.int32, shape, 1)
    outer = lax.broadcasted_iota(jnp.int32, shape, 2)
    subkey = jax.random.fold_in(key, 37)
    values = jax.random.normal(subkey, shape, jnp.float32)
    values = values * (0.5 / math.sqrt(BLK))
    lower_part = jnp.where(outer < inner, values, 0.0)
    return (lower_part + jnp.where(outer == inner, 1.0, 0.0)).astype(jnp.float32)


def shard_levels(key, shape, cuts, smallest, largest):
    def one(axis_at, shards_of):
        draws = jax.random.uniform(jax.random.fold_in(jax.random.fold_in(key, 6), axis_at), (shards_of,), jnp.float32, smallest / len(cuts), largest / len(cuts))
        return jnp.repeat(jnp.exp(draws), shape[axis_at] // shards_of).reshape((-1,) + (1,) * (len(shape) - axis_at - 1))

    loudness = one(*cuts[0])
    for cut in cuts[1:]:
        loudness = loudness * one(*cut)
    return loudness


def gaussian(own_key, dims, scale, bound, cuts=(), dtype=jnp.bfloat16):
    loudness = shard_levels(own_key, dims, cuts, -0.22, 0.18) if cuts else 1.0
    drawn = jax.random.normal(own_key, dims, jnp.float32) * scale * loudness
    return jnp.minimum(jnp.maximum(drawn, -bound), bound).astype(dtype)


def setup_inputs(seed: int = 0) -> dict:
    key_list = jax.random.split(jax.random.key(seed), 5)
    rhs = gaussian(key_list[0], (NRHS, N), 1.0, 6.0, ((1, 256),), jnp.float32)
    pivots = draw_pivots(jax.random.fold_in(key_list[4], 71), 0)
    factor = draw_factor(jax.random.fold_in(key_list[4], 71), 0)
    diag_inv = draw_diag_inv(jax.random.fold_in(key_list[4], 71), 0)
    return dict(rhs=rhs, pivots=pivots, factor=factor, diag_inv=diag_inv)


def reference(rhs, pivots, factor, diag_inv):
    width = NB * BLK
    permuted = jnp.take(rhs, pivots, axis=1)
    full_lower = factor.reshape(width, width)

    def advance(number, solved):
        offset = (number * BLK).astype(jnp.int32)
        block_rows = lax.dynamic_slice_in_dim(full_lower, offset, BLK, 0)
        summed = lax.dot_general(solved, block_rows, (((1,), (1,)), ((), ())), precision=lax.Precision.HIGHEST, preferred_element_type=jnp.float32)
        own_rhs = lax.dynamic_slice_in_dim(permuted, offset, BLK, 1)
        block_inv = lax.dynamic_index_in_dim(diag_inv, number.astype(jnp.int32), 0, keepdims=False)
        fresh = lax.dot_general(own_rhs - summed, block_inv, (((1,), (1,)), ((), ())), precision=lax.Precision.HIGHEST, preferred_element_type=jnp.float32)
        return lax.dynamic_update_slice_in_dim(solved, fresh, offset, 1)

    solved = lax.fori_loop(jnp.int32(0), jnp.int32(NB), advance, jnp.zeros((NRHS, width), jnp.float32))
    return solved.reshape(NRHS, NB * (BLK // CB) // N_COL, N_COL, CB)
```

```python
import functools

import jax
import jax.numpy as jnp
from jax import lax
from jax.experimental import pallas as pl
from jax.experimental.pallas import tpu as pltpu
from jax.sharding import Mesh
from jax.sharding import PartitionSpec as P

QUAD = 4


def dot(a, b, contract):
    return lax.dot_general(
        a,
        b,
        (contract, ((), ())),
        precision=lax.Precision.HIGHEST,
        preferred_element_type=jnp.float32,
    )


def split3(x):
    hi = x.astype(jnp.bfloat16)
    rest = x - hi.astype(jnp.float32)
    mid = rest.astype(jnp.bfloat16)
    lo = (rest - mid.astype(jnp.float32)).astype(jnp.bfloat16)
    return hi, mid, lo


def take_kernel(first_ref, pivots_ref, rhs_ref, out_ref):
    count, source = rhs_ref.shape
    located = pivots_ref[...] - first_ref[0]
    place = lax.broadcasted_iota(jnp.int32, (source, located.shape[1]), 0)
    pick = jnp.where(place == located, 1.0, 0.0).astype(jnp.bfloat16)
    parts = jnp.concatenate(split3(rhs_ref[...]), axis=0)
    got = jnp.dot(parts, pick, preferred_element_type=jnp.float32)
    got = (got[2 * count :] + got[count : 2 * count]) + got[:count]
    pieces, _, length = out_ref.shape
    for n in range(pieces):
        out_ref[n] = got[:, n * length : (n + 1) * length]


def take_columns(rhs, pivots, first, piece_len):
    count, source = rhs.shape
    total = pivots.shape[0]
    step = source
    return pl.pallas_call(
        take_kernel,
        grid=(total // step,),
        in_specs=[
            pl.BlockSpec(memory_space=pltpu.SMEM),
            pl.BlockSpec((1, step), lambda n: (0, n)),
            pl.BlockSpec((count, source), lambda n: (0, 0)),
        ],
        out_specs=pl.BlockSpec((step // piece_len, count, piece_len), lambda n: (n, 0, 0)),
        out_shape=jax.ShapeDtypeStruct((total // piece_len, count, piece_len), jnp.float32),
    )(first.reshape(1), pivots.reshape(1, total), rhs)


def per_device(rhs, pivots, factor, diag_inv):
    my_row = lax.axis_index("row")
    my_quad = lax.axis_index("quad")
    my_i = lax.axis_index("i")
    rows = lax.axis_size("row")
    quads = lax.axis_size("quad")
    core = my_i % 2
    half = my_i // 2
    rhs_count, source_len = rhs.shape
    block_len, _, _, piece_len = factor.shape
    group = rhs_count // rows
    flat = (my_row * quads + my_quad) * QUAD + my_i

    taken = take_columns(rhs, pivots, flat * source_len, piece_len)

    inverse = diag_inv[0]
    lower = factor.reshape(block_len, piece_len)
    scaled = dot(inverse, lower, ((1,), (0,)))
    own_rows = lax.dynamic_slice_in_dim(inverse, my_i * piece_len, piece_len, 0)
    slot = jnp.where(my_quad == my_row, own_rows.T, -scaled)
    slots = lax.all_gather(slot, "row")

    piece = lax.all_to_all(taken, ("quad", "i"), 0, 0, tiled=True).sum(axis=0)
    outgoing = jnp.broadcast_to(
        piece.reshape(rows, 1, group, piece_len), (rows, QUAD, group, piece_len)
    ).reshape(rows * QUAD, group, piece_len)
    incoming = lax.all_to_all(outgoing, ("row", "i"), 0, 0, tiled=True)
    block = incoming.reshape(rows, QUAD, group, piece_len).sum(axis=0)
    block = jnp.moveaxis(block, 0, 1).reshape(group, block_len)
    mine = lax.dynamic_index_in_dim(slots, my_quad, 0, keepdims=False)
    start = dot(block, mine, ((1,), (0,)))

    def pairs(step, flip):
        out = []
        for q in range(quads):
            if step % 2 == 0:
                to = q ^ 1
            else:
                to = q + 1 if q % 2 else q - 1
            if 0 <= to < quads:
                out += [(q * QUAD + i, to * QUAD + (i ^ flip)) for i in range(QUAD)]
        return out

    partner = [(i, i ^ 1) for i in range(QUAD)]
    y = start
    final = start
    later = None
    for step in range(quads - 1):
        part = dot(y, slots[step + 1], ((1,), (1,)))
        if later is not None:
            part = part + later[0]
        rest = None
        if step + 2 < quads:
            rest = dot(
                y, slots[step + 2 :].reshape(-1, piece_len), ((1,), (1,))
            )
            rest = jnp.moveaxis(rest.reshape(group, quads - 2 - step, block_len), 0, 1)
            if later is not None:
                rest = rest + later[1:]
            rest = lax.ppermute(rest, ("quad", "i"), pairs(step, 2))
        part = part.reshape(group, 2, 2, piece_len)
        keep = jnp.where(core == 0, part[:, :, 0], part[:, :, 1])
        give = jnp.where(core == 0, part[:, :, 1], part[:, :, 0])
        both = keep + lax.ppermute(give, "i", partner)
        same = jnp.where(half == 0, both[:, 0], both[:, 1])
        other = jnp.where(half == 0, both[:, 1], both[:, 0])
        y = (
            start
            + lax.ppermute(same, ("quad", "i"), pairs(step, 0))
            + lax.ppermute(other, ("quad", "i"), pairs(step, 2))
        )
        final = jnp.where(my_quad == step + 1, y, final)
        later = rest
    whole = lax.all_to_all(
        jnp.broadcast_to(final[None], (rows, group, piece_len)), "row", 0, 0, tiled=True
    )
    return whole.reshape(rhs_count, 1, 1, piece_len)


def solution(mesh):
    rows, cols = mesh.devices.shape
    grid = Mesh(mesh.devices.reshape(rows, cols // QUAD, QUAD), ("row", "quad", "i"))
    return jax.shard_map(
        per_device,
        mesh=grid,
        in_specs=(
            P(None, ("row", "quad", "i")),
            P(),
            P("row", None, ("quad", "i"), None),
            P("row", None, None),
        ),
        out_specs=P(None, None, ("quad", "i"), None),
        check_vma=False,
    )
```

```python
import functools

import jax
import jax.numpy as jnp
from jax import lax
from jax.experimental import pallas as pl
from jax.experimental.pallas import tpu as pltpu
from jax.sharding import Mesh
from jax.sharding import PartitionSpec as P

QUAD = 4


def dot(a, b, contract):
    return lax.dot_general(
        a,
        b,
        (contract, ((), ())),
        precision=lax.Precision.HIGHEST,
        preferred_element_type=jnp.float32,
    )


def split3(x):
    hi = x.astype(jnp.bfloat16)
    rest = x - hi.astype(jnp.float32)
    mid = rest.astype(jnp.bfloat16)
    lo = (rest - mid.astype(jnp.float32)).astype(jnp.bfloat16)
    return hi, mid, lo


def take_kernel(first_ref, pivots_ref, rhs_ref, out_ref):
    count, source = rhs_ref.shape
    located = pivots_ref[...] - first_ref[0]
    place = lax.broadcasted_iota(jnp.int32, (source, located.shape[1]), 0)
    pick = jnp.where(place == located, 1.0, 0.0).astype(jnp.bfloat16)
    parts = jnp.concatenate(split3(rhs_ref[...]), axis=0)
    got = jnp.dot(parts, pick, preferred_element_type=jnp.float32)
    got = (got[2 * count :] + got[count : 2 * count]) + got[:count]
    pieces, _, length = out_ref.shape
    for n in range(pieces):
        out_ref[n] = got[:, n * length : (n + 1) * length]


def take_columns(rhs, pivots, first, piece_len):
    count, source = rhs.shape
    total = pivots.shape[0]
    step = source
    return pl.pallas_call(
        take_kernel,
        grid=(total // step,),
        in_specs=[
            pl.BlockSpec(memory_space=pltpu.SMEM),
            pl.BlockSpec((1, step), lambda n: (0, n)),
            pl.BlockSpec((count, source), lambda n: (0, 0)),
        ],
        out_specs=pl.BlockSpec((step // piece_len, count, piece_len), lambda n: (n, 0, 0)),
        out_shape=jax.ShapeDtypeStruct((total // piece_len, count, piece_len), jnp.float32),
    )(first.reshape(1), pivots.reshape(1, total), rhs)


def mirrored(quad, i):
    if quad // 2 % 2:
        return quad, i
    return quad ^ 1, i ^ 2


def next_quad(quad, step, quads):
    if step % 2 == 0:
        return quad ^ 1
    turn, side = quad // 2, quad % 2
    turn = turn ^ 1 if step % 4 == 1 else (turn + 1 if turn % 2 else turn - 1) % (quads // 2)
    return 2 * turn + side


def per_device(rhs, pivots, factor, diag_inv):
    my_row = lax.axis_index("row")
    my_quad = lax.axis_index("quad")
    my_i = lax.axis_index("i")
    rows = lax.axis_size("row")
    quads = lax.axis_size("quad")
    turned = my_quad // 2 % 2 == 0
    at_quad = jnp.where(turned, my_quad ^ 1, my_quad)
    at_i = jnp.where(turned, my_i ^ 2, my_i)
    core = at_i % 2
    half = at_i // 2
    rhs_count, source_len = rhs.shape
    block_len, _, _, piece_len = factor.shape
    group = rhs_count // rows
    flat = (my_row * quads + my_quad) * QUAD + my_i
    places = [(q, i) for q in range(quads) for i in range(QUAD)]

    def pairs(move):
        return [(q * QUAD + i, move(q, i)[0] * QUAD + move(q, i)[1]) for q, i in places]

    def mirror(shard):
        there = [(a, b) for a, b in pairs(mirrored) if a != b]
        return jnp.where(turned, lax.ppermute(shard, ("quad", "i"), there), shard)

    lower = mirror(factor.reshape(block_len, piece_len))
    inverse = diag_inv[0]
    scaled = dot(inverse, lower, ((1,), (0,)))
    own_rows = lax.dynamic_slice_in_dim(inverse, at_i * piece_len, piece_len, 0)
    slot = jnp.where(at_quad == my_row, own_rows.T, -scaled)
    slots = lax.all_gather(slot, "row")

    order = pivots.reshape(quads // 2, 4, -1)
    even = lax.broadcasted_iota(jnp.int32, order.shape, 0) % 2 == 0
    order = jnp.where(even, order[:, ::-1], order).reshape(-1)
    taken = take_columns(rhs, order, flat * source_len, piece_len)
    piece = lax.all_to_all(taken, ("quad", "i"), 0, 0, tiled=True).sum(axis=0)
    outgoing = jnp.broadcast_to(
        piece.reshape(rows, 1, group, piece_len), (rows, QUAD, group, piece_len)
    ).reshape(rows * QUAD, group, piece_len)
    incoming = lax.all_to_all(outgoing, ("row", "i"), 0, 0, tiled=True)
    block = incoming.reshape(rows, QUAD, group, piece_len).sum(axis=0)
    block = jnp.where(turned, jnp.concatenate([block[2:], block[:2]]), block)
    block = jnp.moveaxis(block, 0, 1).reshape(group, block_len)
    mine = lax.dynamic_index_in_dim(slots, at_quad, 0, keepdims=False)
    start = dot(block, mine, ((1,), (0,)))

    partner = [(i, i ^ 1) for i in range(QUAD)]
    y = start
    final = start
    later = None
    home = None
    for step in range(quads - 1):
        part = dot(y, slots[step + 1], ((1,), (1,)))
        if later is not None:
            part = part + later[0]
        part = part.reshape(group, 2, 2, piece_len)
        keep = jnp.where(core == 0, part[:, :, 0], part[:, :, 1])
        give = jnp.where(core == 0, part[:, :, 1], part[:, :, 0])
        both = keep + lax.ppermute(give, "i", partner)
        same = jnp.where(half == 0, both[:, 0], both[:, 1])
        other = jnp.where(half == 0, both[:, 1], both[:, 0])
        sent = other[None]
        if step + 2 < quads:
            rest = [
                dot(y, slots[n], ((1,), (1,))) + (0 if later is None else later[n - step - 1])
                for n in range(step + 2, quads)
            ]
            sent = jnp.concatenate(
                [sent] + [r.reshape(group, QUAD, piece_len).transpose(1, 0, 2) for r in rest]
            )
        near = 2 if step % 2 == 0 else 0
        got = lax.ppermute(
            sent, ("quad", "i"), pairs(lambda q, i: (next_quad(q, step, quads), i ^ near))
        )
        far = lax.ppermute(
            same, ("quad", "i"), pairs(lambda q, i: (next_quad(q, step, quads), i ^ 2 ^ near))
        )
        y = start + got[0] + far
        later = [
            got[1 + QUAD * n : 1 + QUAD * (n + 1)].transpose(1, 0, 2).reshape(group, block_len)
            for n in range(quads - 2 - step)
        ]
        final = jnp.where(at_quad == step + 1, y, final)
        if step == quads - 4:
            home = mirror(final)
    final = jnp.where(turned, home, final)
    whole = lax.all_to_all(
        jnp.broadcast_to(final[None], (rows, group, piece_len)), "row", 0, 0, tiled=True
    )
    return whole.reshape(rhs_count, 1, 1, piece_len)


def solution(mesh):
    rows, cols = mesh.devices.shape
    grid = Mesh(mesh.devices.reshape(rows, cols // QUAD, QUAD), ("row", "quad", "i"))
    return jax.shard_map(
        per_device,
        mesh=grid,
        in_specs=(
            P(None, ("row", "quad", "i")),
            P(),
            P("row", None, ("quad", "i"), None),
            P("row", None, None),
        ),
        out_specs=P(None, None, ("quad", "i"), None),
        check_vma=False,
    )
```

```python
import functools

import jax
import jax.numpy as jnp
from jax import lax
from jax.experimental import pallas as pl
from jax.experimental.pallas import tpu as pltpu
from jax.sharding import Mesh
from jax.sharding import PartitionSpec as P

QUAD = 4


def dot(a, b, contract):
    return lax.dot_general(
        a,
        b,
        (contract, ((), ())),
        precision=lax.Precision.HIGHEST,
        preferred_element_type=jnp.float32,
    )


def split3(x):
    hi = x.astype(jnp.bfloat16)
    rest = x - hi.astype(jnp.float32)
    mid = rest.astype(jnp.bfloat16)
    lo = (rest - mid.astype(jnp.float32)).astype(jnp.bfloat16)
    return hi, mid, lo


def take_kernel(first_ref, pivots_ref, rhs_ref, out_ref):
    count, source = rhs_ref.shape
    located = pivots_ref[...] - first_ref[0]
    place = lax.broadcasted_iota(jnp.int32, (source, located.shape[1]), 0)
    pick = jnp.where(place == located, 1.0, 0.0).astype(jnp.bfloat16)
    parts = jnp.concatenate(split3(rhs_ref[...]), axis=0)
    got = jnp.dot(parts, pick, preferred_element_type=jnp.float32)
    got = (got[2 * count :] + got[count : 2 * count]) + got[:count]
    pieces, _, length = out_ref.shape
    for n in range(pieces):
        out_ref[n] = got[:, n * length : (n + 1) * length]


def take_columns(rhs, pivots, first, piece_len):
    count, source = rhs.shape
    total = pivots.shape[0]
    step = source
    return pl.pallas_call(
        take_kernel,
        grid=(total // step,),
        in_specs=[
            pl.BlockSpec(memory_space=pltpu.SMEM),
            pl.BlockSpec((1, step), lambda n: (0, n)),
            pl.BlockSpec((count, source), lambda n: (0, 0)),
        ],
        out_specs=pl.BlockSpec((step // piece_len, count, piece_len), lambda n: (n, 0, 0)),
        out_shape=jax.ShapeDtypeStruct((total // piece_len, count, piece_len), jnp.float32),
    )(first.reshape(1), pivots.reshape(1, total), rhs)


def mirrored(quad, i):
    if quad // 2 % 2:
        return quad, i
    return quad ^ 1, i ^ 2


def next_quad(quad, step, quads):
    if step % 2 == 0:
        return quad ^ 1
    turn, side = quad // 2, quad % 2
    turn = turn ^ 1 if step % 4 == 1 else (turn + 1 if turn % 2 else turn - 1) % (quads // 2)
    return 2 * turn + side


def per_device(rhs, pivots, factor, diag_inv):
    my_row = lax.axis_index("row")
    my_quad = lax.axis_index("quad")
    my_i = lax.axis_index("i")
    rows = lax.axis_size("row")
    quads = lax.axis_size("quad")
    turned = my_quad // 2 % 2 == 0
    at_quad = jnp.where(turned, my_quad ^ 1, my_quad)
    at_i = jnp.where(turned, my_i ^ 2, my_i)
    core = at_i % 2
    half = at_i // 2
    rhs_count, source_len = rhs.shape
    block_len, _, _, piece_len = factor.shape
    group = rhs_count // rows
    flat = (my_row * quads + my_quad) * QUAD + my_i
    places = [(q, i) for q in range(quads) for i in range(QUAD)]

    def pairs(move):
        return [(q * QUAD + i, move(q, i)[0] * QUAD + move(q, i)[1]) for q, i in places]

    def mirror(shard):
        there = [(a, b) for a, b in pairs(mirrored) if a != b]
        return jnp.where(turned, lax.ppermute(shard, ("quad", "i"), there), shard)

    order = pivots.reshape(quads // 2, 4, -1)
    even = lax.broadcasted_iota(jnp.int32, order.shape, 0) % 2 == 0
    order = jnp.where(even, order[:, ::-1], order).reshape(-1)
    taken = take_columns(rhs, order, flat * source_len, piece_len)
    lower, taken = lax.optimization_barrier((mirror(factor.reshape(block_len, piece_len)), taken))
    inverse = diag_inv[0]
    scaled = dot(lower, inverse, ((0,), (1,)))
    own_rows = lax.dynamic_slice_in_dim(inverse, at_i * piece_len, piece_len, 0)
    slot = jnp.where(at_quad == my_row, own_rows, -scaled)
    slots = lax.all_gather(slot, "row")

    piece = lax.all_to_all(taken, ("quad", "i"), 0, 0, tiled=True).sum(axis=0)
    outgoing = jnp.broadcast_to(
        piece.reshape(rows, 1, group, piece_len), (rows, QUAD, group, piece_len)
    ).reshape(rows * QUAD, group, piece_len)
    incoming = lax.all_to_all(outgoing, ("row", "i"), 0, 0, tiled=True)
    slots, incoming = lax.optimization_barrier((slots, incoming))
    block = incoming.reshape(rows, QUAD, group, piece_len).sum(axis=0)
    block = jnp.where(turned, jnp.concatenate([block[2:], block[:2]]), block)
    block = jnp.moveaxis(block, 0, 1).reshape(group, block_len)

    partner = [(i, i ^ 1) for i in range(QUAD)]
    slots2 = (slots, lax.ppermute(slots, "i", partner))

    def in_order(own, other):
        return jnp.where(core == 0, own, other), jnp.where(core == 0, other, own)

    starts = in_order(
        *(
            dot(block, lax.dynamic_index_in_dim(s, at_quad, 0, keepdims=False), ((1,), (1,)))
            for s in slots2
        )
    )
    start = jnp.concatenate(starts, axis=1)
    both = start
    final = start
    later = None
    home = None
    half_len = 2 * piece_len
    for step in range(quads - 1):
        ys = in_order(both[:, :piece_len], both[:, piece_len:])

        def product(n):
            got = dot(ys[0], slots2[0][n], ((1,), (0,))) + dot(ys[1], slots2[1][n], ((1,), (0,)))
            return got if later is None else got + later[n - step - 1]

        part = product(step + 1)
        low, high = part[:, :half_len], part[:, half_len:]
        same = jnp.where(half == 0, low, high)
        other = jnp.where(half == 0, high, low)
        sent = [other]
        for n in range(step + 2, quads):
            more = product(n)
            sent += [more[:, :half_len], more[:, half_len:]]
        near = 2 if step % 2 == 0 else 0
        got = lax.ppermute(
            jnp.stack(sent),
            ("quad", "i"),
            pairs(lambda q, i: (next_quad(q, step, quads), i ^ near)),
        )
        far = lax.ppermute(
            same, ("quad", "i"), pairs(lambda q, i: (next_quad(q, step, quads), i ^ 2 ^ near))
        )
        both = start + got[0] + far
        later = [
            jnp.concatenate([got[1 + 2 * n], got[2 + 2 * n]], axis=1)
            for n in range(quads - 2 - step)
        ]
        final = jnp.where(at_quad == step + 1, both, final)
        if step == quads - 4:
            home = mirror(final)
    final = jnp.where(turned, home, final)
    final = jnp.where(core == 0, final[:, :piece_len], final[:, piece_len:])
    whole = lax.all_to_all(
        jnp.broadcast_to(final[None], (rows, group, piece_len)), "row", 0, 0, tiled=True
    )
    return whole.reshape(rhs_count, 1, 1, piece_len)


def solution(mesh):
    rows, cols = mesh.devices.shape
    grid = Mesh(mesh.devices.reshape(rows, cols // QUAD, QUAD), ("row", "quad", "i"))
    return jax.shard_map(
        per_device,
        mesh=grid,
        in_specs=(
            P(None, ("row", "quad", "i")),
            P(),
            P("row", None, ("quad", "i"), None),
            P("row", None, None),
        ),
        out_specs=P(None, None, ("quad", "i"), None),
        check_vma=False,
    )
```

```python
import functools

import jax
import jax.numpy as jnp
from jax import lax
from jax.experimental import pallas as pl
from jax.experimental.pallas import tpu as pltpu
from jax.sharding import Mesh
from jax.sharding import PartitionSpec as P

QUAD = 4
VMEM_LIMIT = 16 * 2**20


def dot(a, b, contract):
    return lax.dot_general(
        a,
        b,
        (contract, ((), ())),
        precision=lax.Precision.HIGHEST,
        preferred_element_type=jnp.float32,
    )


def split3(x):
    hi = x.astype(jnp.bfloat16)
    rest = x - hi.astype(jnp.float32)
    mid = rest.astype(jnp.bfloat16)
    lo = (rest - mid.astype(jnp.float32)).astype(jnp.bfloat16)
    return hi, mid, lo


def take_kernel(first_ref, pivots_ref, rhs_ref, out_ref):
    count, source = rhs_ref.shape
    located = pivots_ref[...] - first_ref[0]
    place = lax.broadcasted_iota(jnp.int32, (source, located.shape[1]), 0)
    pick = jnp.where(place == located, 1.0, 0.0).astype(jnp.bfloat16)
    parts = jnp.concatenate(split3(rhs_ref[...]), axis=0)
    got = jnp.dot(parts, pick, preferred_element_type=jnp.float32)
    got = (got[2 * count :] + got[count : 2 * count]) + got[:count]
    pieces, _, length = out_ref.shape
    for n in range(pieces):
        out_ref[n] = got[:, n * length : (n + 1) * length]


def take_columns(rhs, pivots, first, piece_len):
    count, source = rhs.shape
    total = pivots.shape[0]
    step = source
    return pl.pallas_call(
        take_kernel,
        grid=(total // step,),
        in_specs=[
            pl.BlockSpec(memory_space=pltpu.SMEM),
            pl.BlockSpec((1, step), lambda n: (0, n)),
            pl.BlockSpec((count, source), lambda n: (0, 0)),
        ],
        out_specs=pl.BlockSpec((step // piece_len, count, piece_len), lambda n: (n, 0, 0)),
        out_shape=jax.ShapeDtypeStruct((total // piece_len, count, piece_len), jnp.float32),
        compiler_params=pltpu.CompilerParams(vmem_limit_bytes=VMEM_LIMIT),
    )(first.reshape(1), pivots.reshape(1, total), rhs)


def split2(x):
    hi = x.astype(jnp.bfloat16)
    return hi, (x - hi.astype(jnp.float32)).astype(jnp.bfloat16)


NN = ((1,), (0,))
NT = ((1,), (1,))


def product(y, hi, mid, contract):
    rows = y.shape[0]
    y_hi, y_mid = split2(y)

    def mul(a, b):
        return lax.dot_general(a, b, (contract, ((), ())), preferred_element_type=jnp.float32)

    wide = mul(jnp.concatenate([y_hi, y_mid], axis=0), hi)
    return wide[:rows] + (wide[rows:] + mul(y_hi, mid))


def prep_kernel(flags_ref, mine_ref, theirs_ref, hi_ref, mid_ref):
    core = flags_ref[0]
    length = mine_ref.shape[1]
    for place, ref in ((core, mine_ref), (1 - core, theirs_ref)):
        at = pl.ds(pl.multiple_of(place * length, length), length)
        hi_ref[0, at, :], mid_ref[0, at, :] = split2(ref[0])


def prepare(flags, mine, theirs):
    blocks, length, width = mine.shape
    shape = (blocks, 2 * length, width)
    block = pl.BlockSpec((1, length, width), lambda n: (n, 0, 0))
    whole = pl.BlockSpec((1, 2 * length, width), lambda n: (n, 0, 0))
    return pl.pallas_call(
        prep_kernel,
        grid=(blocks,),
        in_specs=[pl.BlockSpec(memory_space=pltpu.SMEM), block, block],
        out_specs=[whole, whole],
        out_shape=[pltpu.VMEM(shape, jnp.bfloat16)] * 2,
        compiler_params=pltpu.CompilerParams(vmem_limit_bytes=VMEM_LIMIT),
    )(flags, mine, theirs)


def contributions(step, flags_ref, y, earlier, hi_ref, mid_ref, same_ref, sent_ref):
    half_len = y.shape[1]
    for n in range(step + 1, hi_ref.shape[0]):
        got = product(y, hi_ref[n], mid_ref[n], NN)
        low, high = got[:, :half_len], got[:, half_len:]
        k = n - step - 1
        if earlier is not None:
            low = low + earlier[1 + 2 * k]
            high = high + earlier[2 + 2 * k]
        if k == 0:
            same_ref[...] = jnp.where(flags_ref[1] == 0, low, high)
            sent_ref[0] = jnp.where(flags_ref[1] == 0, high, low)
        else:
            sent_ref[2 * k - 1] = low
            sent_ref[2 * k] = high


def first_kernel(flags_ref, pieces_ref, hi_ref, mid_ref, start_ref, same_ref, sent_ref):
    sums = jnp.sum(pieces_ref[...], axis=0)
    ordered = jnp.where(flags_ref[3] == 1, jnp.concatenate([sums[2:], sums[:2]], axis=0), sums)
    block = jnp.concatenate([ordered[i] for i in range(QUAD)], axis=1)
    own = flags_ref[2]
    start = product(block, hi_ref[own], mid_ref[own], NT)
    start_ref[...] = start
    contributions(0, flags_ref, start, None, hi_ref, mid_ref, same_ref, sent_ref)


def step_kernel(step, flags_ref, start_ref, near_ref, far_ref, final_ref, *rest):
    both = start_ref[...] + near_ref[0] + far_ref[...]
    kept = jnp.where(flags_ref[2] == step, both, final_ref[...])
    if len(rest) == 1:
        rest[0][...] = kept
        return
    hi_ref, mid_ref, kept_ref, same_ref, sent_ref = rest
    kept_ref[...] = kept
    contributions(step, flags_ref, both, near_ref, hi_ref, mid_ref, same_ref, sent_ref)


def call(kernel, flags, args, outs):
    vmem = pl.BlockSpec(memory_space=pltpu.VMEM)
    return pl.pallas_call(
        kernel,
        in_specs=[pl.BlockSpec(memory_space=pltpu.SMEM)] + [vmem] * len(args),
        out_specs=[vmem] * len(outs),
        out_shape=[jax.ShapeDtypeStruct(shape, jnp.float32) for shape in outs],
        compiler_params=pltpu.CompilerParams(vmem_limit_bytes=VMEM_LIMIT),
    )(flags, *args)


def mirrored(quad, i):
    if quad // 2 % 2:
        return quad, i
    return quad ^ 1, i ^ 2


def next_quad(quad, step, quads):
    if step % 2 == 0:
        return quad ^ 1
    turn, side = quad // 2, quad % 2
    turn = turn ^ 1 if step % 4 == 1 else (turn + 1 if turn % 2 else turn - 1) % (quads // 2)
    return 2 * turn + side


def per_device(rhs, pivots, factor, diag_inv):
    my_row = lax.axis_index("row")
    my_quad = lax.axis_index("quad")
    my_i = lax.axis_index("i")
    rows = lax.axis_size("row")
    quads = lax.axis_size("quad")
    turned = my_quad // 2 % 2 == 0
    at_quad = jnp.where(turned, my_quad ^ 1, my_quad)
    at_i = jnp.where(turned, my_i ^ 2, my_i)
    core = at_i % 2
    half = at_i // 2
    rhs_count, source_len = rhs.shape
    block_len, _, _, piece_len = factor.shape
    group = rhs_count // rows
    flat = (my_row * quads + my_quad) * QUAD + my_i
    places = [(q, i) for q in range(quads) for i in range(QUAD)]

    def pairs(move):
        return [(q * QUAD + i, move(q, i)[0] * QUAD + move(q, i)[1]) for q, i in places]

    def mirror(shard):
        there = [(a, b) for a, b in pairs(mirrored) if a != b]
        return jnp.where(turned, lax.ppermute(shard, ("quad", "i"), there), shard)

    order = pivots.reshape(quads // 2, 4, -1)
    even = lax.broadcasted_iota(jnp.int32, order.shape, 0) % 2 == 0
    order = jnp.where(even, order[:, ::-1], order).reshape(-1)
    taken = take_columns(rhs, order, flat * source_len, piece_len)
    lower, taken = lax.optimization_barrier((mirror(factor.reshape(block_len, piece_len)), taken))
    inverse = diag_inv[0]
    scaled = dot(lower, inverse, ((0,), (1,)))
    own_rows = lax.dynamic_slice_in_dim(inverse, at_i * piece_len, piece_len, 0)
    slot = jnp.where(at_quad == my_row, own_rows, -scaled)
    slots = lax.all_gather(slot, "row")

    piece = lax.all_to_all(taken, ("quad", "i"), 0, 0, tiled=True).sum(axis=0)
    outgoing = jnp.broadcast_to(
        piece.reshape(rows, 1, group, piece_len), (rows, QUAD, group, piece_len)
    ).reshape(rows * QUAD, group, piece_len)
    incoming = lax.all_to_all(outgoing, ("row", "i"), 0, 0, tiled=True)
    slots, incoming = lax.optimization_barrier((slots, incoming))
    flags = jnp.stack([core, half, at_quad, turned.astype(jnp.int32)]).astype(jnp.int32)
    partner = [(i, i ^ 1) for i in range(QUAD)]
    hi, mid = prepare(flags, slots, lax.ppermute(slots, "i", partner))
    wide = (group, 2 * piece_len)

    def sent_shape(step):
        return (2 * (quads - 2 - step) + 1, *wide)

    start, same, sent = call(
        first_kernel,
        flags,
        (incoming.reshape(rows, QUAD, group, piece_len), hi, mid),
        (wide, wide, sent_shape(0)),
    )
    final = start
    for step in range(quads - 1):
        near = 2 if step % 2 == 0 else 0
        far_to = pairs(lambda q, i: (next_quad(q, step, quads), i ^ 2 ^ near))
        near_to = pairs(lambda q, i: (next_quad(q, step, quads), i ^ near))
        far = lax.ppermute(same, ("quad", "i"), far_to)
        got = lax.ppermute(sent, ("quad", "i"), near_to)
        args, outs = (start, got, far, final), (wide,)
        if step + 2 < quads:
            args, outs = (*args, hi, mid), (wide, wide, sent_shape(step + 1))
        final, *rest = call(functools.partial(step_kernel, step + 1), flags, args, outs)
        if rest:
            same, sent = rest
        if step == quads - 4:
            home = mirror(final)
    final = jnp.where(turned, home, final)
    final = jnp.where(core == 0, final[:, :piece_len], final[:, piece_len:])
    whole = lax.all_to_all(
        jnp.broadcast_to(final[None], (rows, group, piece_len)), "row", 0, 0, tiled=True
    )
    return whole.reshape(rhs_count, 1, 1, piece_len)


def solution(mesh):
    rows, cols = mesh.devices.shape
    grid = Mesh(mesh.devices.reshape(rows, cols // QUAD, QUAD), ("row", "quad", "i"))
    return jax.shard_map(
        per_device,
        mesh=grid,
        in_specs=(
            P(None, ("row", "quad", "i")),
            P(),
            P("row", None, ("quad", "i"), None),
            P("row", None, None),
        ),
        out_specs=P(None, None, ("quad", "i"), None),
        check_vma=False,
    )
```

```python
import functools

import jax
import jax.numpy as jnp
from jax import lax
from jax.experimental import pallas as pl
from jax.experimental.pallas import tpu as pltpu
from jax.sharding import Mesh
from jax.sharding import PartitionSpec as P

QUAD = 4
VMEM_LIMIT = 16 * 2**20


def dot(a, b, contract):
    return lax.dot_general(
        a,
        b,
        (contract, ((), ())),
        precision=lax.Precision.HIGHEST,
        preferred_element_type=jnp.float32,
    )


def split3(x):
    hi = x.astype(jnp.bfloat16)
    rest = x - hi.astype(jnp.float32)
    mid = rest.astype(jnp.bfloat16)
    lo = (rest - mid.astype(jnp.float32)).astype(jnp.bfloat16)
    return hi, mid, lo


def take_kernel(first_ref, pivots_ref, rhs_ref, out_ref):
    count, source = rhs_ref.shape
    located = pivots_ref[...] - first_ref[0]
    place = lax.broadcasted_iota(jnp.int32, (source, located.shape[1]), 0)
    pick = jnp.where(place == located, 1.0, 0.0).astype(jnp.bfloat16)
    parts = jnp.concatenate(split3(rhs_ref[...]), axis=0)
    got = jnp.dot(parts, pick, preferred_element_type=jnp.float32)
    got = (got[2 * count :] + got[count : 2 * count]) + got[:count]
    pieces, _, length = out_ref.shape
    for n in range(pieces):
        out_ref[n] = got[:, n * length : (n + 1) * length]


def take_columns(rhs, pivots, first, piece_len):
    count, source = rhs.shape
    total = pivots.shape[0]
    step = source
    return pl.pallas_call(
        take_kernel,
        grid=(total // step,),
        in_specs=[
            pl.BlockSpec(memory_space=pltpu.SMEM),
            pl.BlockSpec((1, step), lambda n: (0, n)),
            pl.BlockSpec((count, source), lambda n: (0, 0)),
        ],
        out_specs=pl.BlockSpec((step // piece_len, count, piece_len), lambda n: (n, 0, 0)),
        out_shape=jax.ShapeDtypeStruct((total // piece_len, count, piece_len), jnp.float32),
        compiler_params=pltpu.CompilerParams(vmem_limit_bytes=VMEM_LIMIT),
    )(first.reshape(1), pivots.reshape(1, total), rhs)


def split2(x):
    hi = x.astype(jnp.bfloat16)
    return hi, (x - hi.astype(jnp.float32)).astype(jnp.bfloat16)


NN = ((1,), (0,))
NT = ((1,), (1,))


def product(y, hi, mid, contract):
    rows = y.shape[0]
    y_hi, y_mid = split2(y)

    def mul(a, b):
        return lax.dot_general(a, b, (contract, ((), ())), preferred_element_type=jnp.float32)

    wide = mul(jnp.concatenate([y_hi, y_mid], axis=0), hi)
    return wide[:rows] + (wide[rows:] + mul(y_hi, mid))


def prep_kernel(distances, flags_ref, *refs):
    count = len(distances)
    mine, theirs = refs[:count], refs[count:-2]
    hi_ref, mid_ref = refs[-2:]
    rows = hi_ref.shape[0]
    length = mine[0].shape[-2]
    core = flags_ref[0]

    def put(row, place, value):
        at = pl.ds(pl.multiple_of(place * length, length), length)
        hi_ref[row, at, :], mid_ref[row, at, :] = split2(value)

    for n, distance in enumerate(distances):
        put((flags_ref[4] + distance) % rows, core, mine[n][...])
    n = 0
    for ref in theirs:
        for k in range(ref.shape[0]):
            put((flags_ref[4] + distances[n]) % rows, 1 - core, ref[k])
            n += 1


def prepare(flags, distances, mine, theirs):
    length, width = mine[0].shape
    shape = (len(distances), 2 * length, width)
    vmem = pl.BlockSpec(memory_space=pltpu.VMEM)
    return pl.pallas_call(
        functools.partial(prep_kernel, distances),
        in_specs=[pl.BlockSpec(memory_space=pltpu.SMEM)] + [vmem] * (len(mine) + len(theirs)),
        out_specs=[vmem, vmem],
        out_shape=[pltpu.VMEM(shape, jnp.bfloat16)] * 2,
        compiler_params=pltpu.CompilerParams(vmem_limit_bytes=VMEM_LIMIT),
    )(flags, *mine, *theirs)


def contributions(step, flags_ref, y, earlier, hi_ref, mid_ref, same_ref, sent_ref):
    half_len = y.shape[1]
    for n in range(step + 1, hi_ref.shape[0]):
        got = product(y, hi_ref[n], mid_ref[n], NN)
        low, high = got[:, :half_len], got[:, half_len:]
        k = n - step - 1
        if earlier is not None:
            low = low + earlier[1 + 2 * k]
            high = high + earlier[2 + 2 * k]
        if k == 0:
            same_ref[...] = jnp.where(flags_ref[1] == 0, low, high)
            sent_ref[0] = jnp.where(flags_ref[1] == 0, high, low)
        else:
            sent_ref[2 * k - 1] = low
            sent_ref[2 * k] = high


def first_kernel(flags_ref, pieces_ref, hi_ref, mid_ref, start_ref, same_ref, sent_ref):
    sums = jnp.sum(pieces_ref[...], axis=0)
    ordered = jnp.where(flags_ref[3] == 1, jnp.concatenate([sums[2:], sums[:2]], axis=0), sums)
    block = jnp.concatenate([ordered[i] for i in range(QUAD)], axis=1)
    own = flags_ref[2]
    start = product(block, hi_ref[own], mid_ref[own], NT)
    start_ref[...] = start
    contributions(0, flags_ref, start, None, hi_ref, mid_ref, same_ref, sent_ref)


def step_kernel(step, flags_ref, start_ref, near_ref, far_ref, final_ref, *rest):
    both = start_ref[...] + near_ref[0] + far_ref[...]
    kept = jnp.where(flags_ref[2] == step, both, final_ref[...])
    if len(rest) == 1:
        rest[0][...] = kept
        return
    hi_ref, mid_ref, kept_ref, same_ref, sent_ref = rest
    kept_ref[...] = kept
    contributions(step, flags_ref, both, near_ref, hi_ref, mid_ref, same_ref, sent_ref)


def call(kernel, flags, args, outs):
    vmem = pl.BlockSpec(memory_space=pltpu.VMEM)
    return pl.pallas_call(
        kernel,
        in_specs=[pl.BlockSpec(memory_space=pltpu.SMEM)] + [vmem] * len(args),
        out_specs=[vmem] * len(outs),
        out_shape=[jax.ShapeDtypeStruct(shape, jnp.float32) for shape in outs],
        compiler_params=pltpu.CompilerParams(vmem_limit_bytes=VMEM_LIMIT),
    )(flags, *args)


def mirrored(quad, i):
    if quad // 2 % 2:
        return quad, i
    return quad ^ 1, i ^ 2


def next_quad(quad, step, quads):
    if step % 2 == 0:
        return quad ^ 1
    turn, side = quad // 2, quad % 2
    turn = turn ^ 1 if step % 4 == 1 else (turn + 1 if turn % 2 else turn - 1) % (quads // 2)
    return 2 * turn + side


def per_device(rhs, pivots, factor, diag_inv):
    my_row = lax.axis_index("row")
    my_quad = lax.axis_index("quad")
    my_i = lax.axis_index("i")
    rows = lax.axis_size("row")
    quads = lax.axis_size("quad")
    turned = my_quad // 2 % 2 == 0
    at_quad = jnp.where(turned, my_quad ^ 1, my_quad)
    at_i = jnp.where(turned, my_i ^ 2, my_i)
    core = at_i % 2
    half = at_i // 2
    rhs_count, source_len = rhs.shape
    block_len, _, _, piece_len = factor.shape
    group = rhs_count // rows
    flat = (my_row * quads + my_quad) * QUAD + my_i
    places = [(q, i) for q in range(quads) for i in range(QUAD)]

    def pairs(move):
        return [(q * QUAD + i, move(q, i)[0] * QUAD + move(q, i)[1]) for q, i in places]

    def mirror(shard):
        there = [(a, b) for a, b in pairs(mirrored) if a != b]
        return jnp.where(turned, lax.ppermute(shard, ("quad", "i"), there), shard)

    order = pivots.reshape(quads // 2, 4, -1)
    even = lax.broadcasted_iota(jnp.int32, order.shape, 0) % 2 == 0
    order = jnp.where(even, order[:, ::-1], order).reshape(-1)
    taken = take_columns(rhs, order, flat * source_len, piece_len)
    lower, taken = lax.optimization_barrier((mirror(factor.reshape(block_len, piece_len)), taken))
    inverse = diag_inv[0]
    scaled = dot(lower, inverse, ((0,), (1,)))
    own_rows = lax.dynamic_slice_in_dim(inverse, at_i * piece_len, piece_len, 0)
    slot = jnp.where(at_quad == my_row, own_rows, -scaled)

    def shift(shard, by):
        return lax.ppermute(shard, "row", [(r, (r + by) % rows) for r in range(rows)])

    partner = [(i, i ^ 1) for i in range(QUAD)]
    first = [shift(slot, 2), shift(slot, -2), shift(slot, 1), shift(slot, -1)]
    piece = lax.all_to_all(taken, ("quad", "i"), 0, 0, tiled=True).sum(axis=0)
    piece, *first = lax.optimization_barrier((piece, *first))
    second = [shift(first[0], 2), shift(first[0], 1), shift(first[1], -1)]
    distances = (0, -2, 2, -1, 1, -4, -3, 3)
    near_rows = [slot, *first]
    theirs = [lax.ppermute(jnp.stack(near_rows), "i", partner)]
    outgoing = jnp.broadcast_to(
        piece.reshape(rows, 1, group, piece_len), (rows, QUAD, group, piece_len)
    ).reshape(rows * QUAD, group, piece_len)
    incoming = lax.all_to_all(outgoing, ("row", "i"), 0, 0, tiled=True)
    incoming, *second = lax.optimization_barrier((incoming, *second))
    theirs.append(lax.ppermute(jnp.stack(second), "i", partner))
    flags = jnp.stack([core, half, at_quad, turned.astype(jnp.int32), my_row]).astype(jnp.int32)
    hi, mid = prepare(flags, distances, near_rows + second, theirs)
    wide = (group, 2 * piece_len)

    def sent_shape(step):
        return (2 * (quads - 2 - step) + 1, *wide)

    start, same, sent = call(
        first_kernel,
        flags,
        (incoming.reshape(rows, QUAD, group, piece_len), hi, mid),
        (wide, wide, sent_shape(0)),
    )
    final = start
    for step in range(quads - 1):
        near = 2 if step % 2 == 0 else 0
        far_to = pairs(lambda q, i: (next_quad(q, step, quads), i ^ 2 ^ near))
        near_to = pairs(lambda q, i: (next_quad(q, step, quads), i ^ near))
        far = lax.ppermute(same, ("quad", "i"), far_to)
        got = lax.ppermute(sent, ("quad", "i"), near_to)
        args, outs = (start, got, far, final), (wide,)
        if step + 2 < quads:
            args, outs = (*args, hi, mid), (wide, wide, sent_shape(step + 1))
        final, *rest = call(functools.partial(step_kernel, step + 1), flags, args, outs)
        if rest:
            same, sent = rest
        if step == quads - 4:
            home = mirror(final)
    final = jnp.where(turned, home, final)
    final = jnp.where(core == 0, final[:, :piece_len], final[:, piece_len:])
    whole = lax.all_to_all(
        jnp.broadcast_to(final[None], (rows, group, piece_len)), "row", 0, 0, tiled=True
    )
    return whole.reshape(rhs_count, 1, 1, piece_len)


def solution(mesh):
    rows, cols = mesh.devices.shape
    grid = Mesh(mesh.devices.reshape(rows, cols // QUAD, QUAD), ("row", "quad", "i"))
    return jax.shard_map(
        per_device,
        mesh=grid,
        in_specs=(
            P(None, ("row", "quad", "i")),
            P(),
            P("row", None, ("quad", "i"), None),
            P("row", None, None),
        ),
        out_specs=P(None, None, ("quad", "i"), None),
        check_vma=False,
    )
```

```python
import functools

import jax
import jax.numpy as jnp
from jax import lax
from jax.experimental import pallas as pl
from jax.experimental.pallas import tpu as pltpu
from jax.sharding import Mesh
from jax.sharding import PartitionSpec as P

QUAD = 4
VMEM_LIMIT = 16 * 2**20


def dot(a, b, contract):
    return lax.dot_general(
        a,
        b,
        (contract, ((), ())),
        precision=lax.Precision.HIGHEST,
        preferred_element_type=jnp.float32,
    )


def split3(x):
    hi = x.astype(jnp.bfloat16)
    rest = x - hi.astype(jnp.float32)
    mid = rest.astype(jnp.bfloat16)
    lo = (rest - mid.astype(jnp.float32)).astype(jnp.bfloat16)
    return hi, mid, lo


def take_kernel(first_ref, pivots_ref, rhs_ref, out_ref):
    count, source = rhs_ref.shape
    located = pivots_ref[...] - first_ref[0]
    place = lax.broadcasted_iota(jnp.int32, (source, located.shape[1]), 0)
    pick = jnp.where(place == located, 1.0, 0.0).astype(jnp.bfloat16)
    parts = jnp.concatenate(split3(rhs_ref[...]), axis=0)
    got = jnp.dot(parts, pick, preferred_element_type=jnp.float32)
    got = (got[2 * count :] + got[count : 2 * count]) + got[:count]
    pieces, _, length = out_ref.shape
    for n in range(pieces):
        out_ref[n] = got[:, n * length : (n + 1) * length]


def take_columns(rhs, pivots, first, piece_len):
    count, source = rhs.shape
    total = pivots.shape[0]
    step = source
    return pl.pallas_call(
        take_kernel,
        grid=(total // step,),
        in_specs=[
            pl.BlockSpec(memory_space=pltpu.SMEM),
            pl.BlockSpec((1, step), lambda n: (0, n)),
            pl.BlockSpec((count, source), lambda n: (0, 0)),
        ],
        out_specs=pl.BlockSpec((step // piece_len, count, piece_len), lambda n: (n, 0, 0)),
        out_shape=jax.ShapeDtypeStruct((total // piece_len, count, piece_len), jnp.float32),
        compiler_params=pltpu.CompilerParams(vmem_limit_bytes=VMEM_LIMIT),
    )(first.reshape(1), pivots.reshape(1, total), rhs)


def split2(x):
    hi = x.astype(jnp.bfloat16)
    return hi, (x - hi.astype(jnp.float32)).astype(jnp.bfloat16)


NN = ((1,), (0,))
NT = ((1,), (1,))


def product(y, hi, mid, contract):
    rows = y.shape[0]
    y_hi, y_mid = split2(y)

    def mul(a, b):
        return lax.dot_general(a, b, (contract, ((), ())), preferred_element_type=jnp.float32)

    wide = mul(jnp.concatenate([y_hi, y_mid], axis=0), hi)
    return wide[:rows] + (wide[rows:] + mul(y_hi, mid))


def prep_kernel(distances, flags_ref, *refs):
    count = len(distances)
    mine, theirs = refs[:count], refs[count : 2 * count]
    hi_ref, mid_ref = refs[-2:]
    rows = hi_ref.shape[0]
    length = mine[0].shape[-2]
    core = flags_ref[0]

    def put(row, place, value):
        at = pl.ds(pl.multiple_of(place * length, length), length)
        hi_ref[row, at, :], mid_ref[row, at, :] = split2(value)

    for n, distance in enumerate(distances):
        row = lax.rem(flags_ref[3] + (distance + rows), rows)
        put(row, core, mine[n][...])
        put(row, 1 - core, theirs[n][...])


def prepare(flags, distances, mine, theirs):
    length, width = mine[0].shape
    shape = (len(distances), 2 * length, width)
    vmem = pl.BlockSpec(memory_space=pltpu.VMEM)
    return pl.pallas_call(
        functools.partial(prep_kernel, distances),
        in_specs=[pl.BlockSpec(memory_space=pltpu.SMEM)] + [vmem] * (len(mine) + len(theirs)),
        out_specs=[vmem, vmem],
        out_shape=[pltpu.VMEM(shape, jnp.bfloat16)] * 2,
        compiler_params=pltpu.CompilerParams(vmem_limit_bytes=VMEM_LIMIT),
    )(flags, *mine, *theirs)


def contributions(step, flags_ref, y, earlier, hi_ref, mid_ref, same_ref, sent_ref):
    half_len = y.shape[1]
    for n in range(step + 1, hi_ref.shape[0]):
        got = product(y, hi_ref[n], mid_ref[n], NN)
        low, high = got[:, :half_len], got[:, half_len:]
        k = n - step - 1
        if earlier is not None:
            low = low + earlier[1 + 2 * k]
            high = high + earlier[2 + 2 * k]
        if k == 0:
            same_ref[...] = jnp.where(flags_ref[1] == 0, low, high)
            sent_ref[0] = jnp.where(flags_ref[1] == 0, high, low)
        else:
            sent_ref[2 * k - 1] = low
            sent_ref[2 * k] = high


def first_kernel(flags_ref, pieces_ref, hi_ref, mid_ref, start_ref, same_ref, sent_ref):
    sums = jnp.sum(pieces_ref[...], axis=0)
    block = jnp.concatenate([sums[i] for i in range(QUAD)], axis=1)
    own = flags_ref[2]
    start = product(block, hi_ref[own], mid_ref[own], NT)
    start_ref[...] = start
    contributions(0, flags_ref, start, None, hi_ref, mid_ref, same_ref, sent_ref)


def step_kernel(step, flags_ref, start_ref, near_ref, far_ref, final_ref, *rest):
    both = start_ref[...] + near_ref[0] + far_ref[...]
    kept = jnp.where(flags_ref[2] == step, both, final_ref[...])
    if len(rest) == 1:
        rest[0][...] = kept
        return
    hi_ref, mid_ref, kept_ref, same_ref, sent_ref = rest
    kept_ref[...] = kept
    contributions(step, flags_ref, both, near_ref, hi_ref, mid_ref, same_ref, sent_ref)


def call(kernel, flags, args, outs):
    vmem = pl.BlockSpec(memory_space=pltpu.VMEM)
    return pl.pallas_call(
        kernel,
        in_specs=[pl.BlockSpec(memory_space=pltpu.SMEM)] + [vmem] * len(args),
        out_specs=[vmem] * len(outs),
        out_shape=[jax.ShapeDtypeStruct(shape, jnp.float32) for shape in outs],
        compiler_params=pltpu.CompilerParams(vmem_limit_bytes=VMEM_LIMIT),
    )(flags, *args)


def next_quad(quad, step, quads):
    if step % 2 == 0:
        return quad ^ 1
    return (quad + (1 if quad % 2 else -1)) % quads


def per_device(rhs, pivots, factor, diag_inv):
    my_row = lax.axis_index("row")
    my_quad = lax.axis_index("quad")
    my_i = lax.axis_index("i")
    rows = lax.axis_size("row")
    quads = lax.axis_size("quad")
    core = my_i % 2
    half = my_i // 2
    rhs_count, source_len = rhs.shape
    block_len, _, _, piece_len = factor.shape
    group = rhs_count // rows
    flat = (my_row * quads + my_quad) * QUAD + my_i
    places = [(q, i) for q in range(quads) for i in range(QUAD)]

    def pairs(move):
        return [(q * QUAD + i, move(q, i)[0] * QUAD + move(q, i)[1]) for q, i in places]

    lower = factor.reshape(block_len, piece_len)
    inverse = diag_inv[0]
    scaled = dot(lower, inverse, ((0,), (1,)))
    own_rows = lax.dynamic_slice_in_dim(inverse, my_i * piece_len, piece_len, 0)
    slot = jnp.where(my_quad == my_row, own_rows, -scaled)

    def shift(shard, by):
        return lax.ppermute(shard, "row", [(r, (r + by) % rows) for r in range(rows)])

    partner = [(i, i ^ 1) for i in range(QUAD)]
    first = [shift(slot, 2), shift(slot, -2), shift(slot, 1), shift(slot, -1)]
    taken = take_columns(rhs, pivots, flat * source_len, piece_len)
    piece = lax.all_to_all(taken, ("quad", "i"), 0, 0, tiled=True).sum(axis=0)
    second = [shift(first[0], 2), shift(first[0], 1), shift(first[1], -1)]
    distances = (0, -2, 2, -1, 1, -4, -3, 3)
    near_rows = [slot, *first]
    theirs = [lax.ppermute(rows_of, "i", partner) for rows_of in near_rows]
    outgoing = jnp.broadcast_to(
        piece.reshape(rows, 1, group, piece_len), (rows, QUAD, group, piece_len)
    ).reshape(rows * QUAD, group, piece_len)
    incoming = lax.all_to_all(outgoing, ("row", "i"), 0, 0, tiled=True)
    incoming, *second = lax.optimization_barrier((incoming, *second))
    theirs += [lax.ppermute(rows_of, "i", partner) for rows_of in second]
    flags = jnp.stack([core, half, my_quad, my_row]).astype(jnp.int32)
    hi, mid = prepare(flags, distances, near_rows + second, theirs)
    wide = (group, 2 * piece_len)

    def sent_shape(step):
        return (2 * (quads - 2 - step) + 1, *wide)

    start, same, sent = call(
        first_kernel,
        flags,
        (incoming.reshape(rows, QUAD, group, piece_len), hi, mid),
        (wide, wide, sent_shape(0)),
    )
    final = start
    for step in range(quads - 1):
        far_to = pairs(lambda q, i: (next_quad(q, step, quads), i))
        near_to = pairs(lambda q, i: (next_quad(q, step, quads), i ^ 2))
        far = lax.ppermute(same, ("quad", "i"), far_to)
        got = lax.ppermute(sent, ("quad", "i"), near_to)
        args, outs = (start, got, far, final), (wide,)
        if step + 2 < quads:
            args, outs = (*args, hi, mid), (wide, wide, sent_shape(step + 1))
        final, *rest = call(functools.partial(step_kernel, step + 1), flags, args, outs)
        if rest:
            same, sent = rest
    final = jnp.where(core == 0, final[:, :piece_len], final[:, piece_len:])
    whole = lax.all_to_all(
        jnp.broadcast_to(final[None], (rows, group, piece_len)), "row", 0, 0, tiled=True
    )
    return whole.reshape(rhs_count, 1, 1, piece_len)


def solution(mesh):
    rows, cols = mesh.devices.shape
    grid = Mesh(mesh.devices.reshape(rows, cols // QUAD, QUAD), ("row", "quad", "i"))
    return jax.shard_map(
        per_device,
        mesh=grid,
        in_specs=(
            P(None, ("row", "quad", "i")),
            P(),
            P("row", None, ("quad", "i"), None),
            P("row", None, None),
        ),
        out_specs=P(None, None, ("quad", "i"), None),
        check_vma=False,
    )
```

```python
import functools

import jax
import jax.numpy as jnp
from jax import lax
from jax.experimental import pallas as pl
from jax.experimental.pallas import tpu as pltpu
from jax.sharding import Mesh
from jax.sharding import PartitionSpec as P


QUAD = 4
VMEM_LIMIT = 16 * 2**20


def dot(a, b, contract):
    return lax.dot_general(
        a,
        b,
        (contract, ((), ())),
        precision=lax.Precision.HIGHEST,
        preferred_element_type=jnp.float32,
    )


def split3(x):
    hi = x.astype(jnp.bfloat16)
    rest = x - hi.astype(jnp.float32)
    mid = rest.astype(jnp.bfloat16)
    lo = (rest - mid.astype(jnp.float32)).astype(jnp.bfloat16)
    return hi, mid, lo


def take_kernel(first_ref, pivots_ref, rhs_ref, out_ref):
    count, source = rhs_ref.shape
    located = pivots_ref[...] - first_ref[0]
    place = lax.broadcasted_iota(jnp.int32, (source, located.shape[1]), 0)
    pick = jnp.where(place == located, 1.0, 0.0).astype(jnp.bfloat16)
    parts = jnp.concatenate(split3(rhs_ref[...]), axis=0)
    got = jnp.dot(parts, pick, preferred_element_type=jnp.float32)
    got = (got[2 * count :] + got[count : 2 * count]) + got[:count]
    pieces, _, length = out_ref.shape
    for n in range(pieces):
        out_ref[n] = got[:, n * length : (n + 1) * length]


def take_columns(rhs, pivots, first, piece_len):
    count, source = rhs.shape
    total = pivots.shape[0]
    step = source
    return pl.pallas_call(
        take_kernel,
        grid=(total // step,),
        in_specs=[
            pl.BlockSpec(memory_space=pltpu.SMEM),
            pl.BlockSpec((1, step), lambda n: (0, n)),
            pl.BlockSpec((count, source), lambda n: (0, 0)),
        ],
        out_specs=pl.BlockSpec((step // piece_len, count, piece_len), lambda n: (n, 0, 0)),
        out_shape=jax.ShapeDtypeStruct((total // piece_len, count, piece_len), jnp.float32),
        compiler_params=pltpu.CompilerParams(vmem_limit_bytes=VMEM_LIMIT),
    )(first.reshape(1), pivots.reshape(1, total), rhs)


def split2(x):
    hi = x.astype(jnp.bfloat16)
    return hi, (x - hi.astype(jnp.float32)).astype(jnp.bfloat16)


NN = ((1,), (0,))
NT = ((1,), (1,))


def product(y, hi, mid, contract):
    rows = y.shape[0]
    y_hi, y_mid = split2(y)

    def mul(a, b):
        return lax.dot_general(a, b, (contract, ((), ())), preferred_element_type=jnp.float32)

    wide = mul(jnp.concatenate([y_hi, y_mid], axis=0), hi)
    return wide[:rows] + (wide[rows:] + mul(y_hi, mid))


def prep_kernel(parts, flags_ref, *refs):
    count = len(parts)
    mine, theirs = refs[:count], refs[count : 2 * count]
    hi_ref, mid_ref = refs[-2:]
    rows = hi_ref.shape[0]
    length = mine[0].shape[0]
    core = flags_ref[0]

    def put(row, place, offset, value):
        start = pl.multiple_of(place * length + offset, value.shape[0])
        at = pl.ds(start, value.shape[0])
        hi_ref[row, at, :], mid_ref[row, at, :] = split2(value)

    for n, (distance, offset) in enumerate(parts):
        row = lax.rem(flags_ref[3] + (distance + rows), rows)
        put(row, core, offset, mine[n][...])
        put(row, 1 - core, offset, theirs[n][...])


def prepare(flags, rows, parts, mine, theirs):
    length, width = mine[0].shape
    shape = (rows, 2 * length, width)
    vmem = pl.BlockSpec(memory_space=pltpu.VMEM)
    return pl.pallas_call(
        functools.partial(prep_kernel, parts),
        in_specs=[pl.BlockSpec(memory_space=pltpu.SMEM)] + [vmem] * (len(mine) + len(theirs)),
        out_specs=[vmem, vmem],
        out_shape=[pltpu.VMEM(shape, jnp.bfloat16)] * 2,
        compiler_params=pltpu.CompilerParams(vmem_limit_bytes=VMEM_LIMIT),
    )(flags, *mine, *theirs)


def contributions(step, flags_ref, y, earlier, hi_ref, mid_ref, same_ref, sent_ref):
    half_len = y.shape[1]
    for n in range(step + 1, hi_ref.shape[0]):
        got = product(y, hi_ref[n], mid_ref[n], NN)
        low, high = got[:, :half_len], got[:, half_len:]
        k = n - step - 1
        if earlier is not None:
            low = low + earlier[1 + 2 * k]
            high = high + earlier[2 + 2 * k]
        if k == 0:
            same_ref[...] = jnp.where(flags_ref[1] == 0, low, high)
            sent_ref[0] = jnp.where(flags_ref[1] == 0, high, low)
        else:
            sent_ref[2 * k - 1] = low
            sent_ref[2 * k] = high


def first_kernel(flags_ref, pieces_ref, hi_ref, mid_ref, start_ref, same_ref, sent_ref):
    sums = jnp.sum(pieces_ref[...], axis=0)
    block = jnp.concatenate([sums[i] for i in range(QUAD)], axis=1)
    own = flags_ref[2]
    start = product(block, hi_ref[own], mid_ref[own], NT)
    start_ref[...] = start
    contributions(0, flags_ref, start, None, hi_ref, mid_ref, same_ref, sent_ref)


def step_kernel(step, flags_ref, start_ref, near_ref, far_ref, final_ref, *rest):
    both = start_ref[...] + near_ref[0] + far_ref[...]
    kept = jnp.where(flags_ref[2] == step, both, final_ref[...])
    if len(rest) == 1:
        rest[0][...] = kept
        return
    hi_ref, mid_ref, kept_ref, same_ref, sent_ref = rest
    kept_ref[...] = kept
    contributions(step, flags_ref, both, near_ref, hi_ref, mid_ref, same_ref, sent_ref)


def call(kernel, flags, args, outs):
    vmem = pl.BlockSpec(memory_space=pltpu.VMEM)
    return pl.pallas_call(
        kernel,
        in_specs=[pl.BlockSpec(memory_space=pltpu.SMEM)] + [vmem] * len(args),
        out_specs=[vmem] * len(outs),
        out_shape=[jax.ShapeDtypeStruct(shape, jnp.float32) for shape in outs],
        compiler_params=pltpu.CompilerParams(vmem_limit_bytes=VMEM_LIMIT),
    )(flags, *args)


def next_quad(quad, step, quads):
    if step % 2 == 0:
        return quad ^ 1
    return (quad + (1 if quad % 2 else -1)) % quads


def solve(rhs, pivots, factor, diag_inv):
    my_row = lax.axis_index("row")
    my_quad = lax.axis_index("quad")
    my_i = lax.axis_index("i")
    rows = lax.axis_size("row")
    quads = lax.axis_size("quad")
    core = my_i % 2
    half = my_i // 2
    rhs_count, source_len = rhs.shape
    block_len, _, _, piece_len = factor.shape
    group = rhs_count // rows
    flat = (my_row * quads + my_quad) * QUAD + my_i
    places = [(q, i) for q in range(quads) for i in range(QUAD)]

    def pairs(move):
        return [(q * QUAD + i, move(q, i)[0] * QUAD + move(q, i)[1]) for q, i in places]

    lower = factor.reshape(block_len, piece_len)
    inverse = diag_inv[0]
    scaled = dot(lower, inverse, ((0,), (1,)))
    own_rows = lax.dynamic_slice_in_dim(inverse, my_i * piece_len, piece_len, 0)
    slot = jnp.where(my_quad == my_row, own_rows, -scaled)

    def shift(shard, by):
        return lax.ppermute(shard, "row", [(r, (r + by) % rows) for r in range(rows)])

    partner = [(i, i ^ 1) for i in range(QUAD)]
    first = [shift(slot, 2), shift(slot, -2)]
    first += [shift(slot, 1), shift(slot, -1)]
    taken = take_columns(rhs, pivots, flat * source_len, piece_len)
    spread = lax.all_to_all(taken, ("quad", "i"), 0, 0, tiled=True)
    piece = spread.sum(axis=0)
    cut = piece_len // 2
    second = [
        shift(first[0][:cut], 2),
        shift(first[1][cut:], -2),
        shift(first[0], 1),
        shift(first[1], -1),
    ]
    parts = ((0, 0), (-2, 0), (2, 0), (-1, 0), (1, 0), (4, 0), (4, cut), (-3, 0), (3, 0))
    near_rows = [slot, *first]
    theirs = [lax.ppermute(rows_of, "i", partner) for rows_of in near_rows]
    outgoing = jnp.broadcast_to(
        piece.reshape(rows, 1, group, piece_len), (rows, QUAD, group, piece_len)
    ).reshape(rows * QUAD, group, piece_len)
    incoming = lax.all_to_all(outgoing, ("row", "i"), 0, 0, tiled=True)
    incoming, *second = lax.optimization_barrier((incoming, *second))
    theirs += [lax.ppermute(rows_of, "i", partner) for rows_of in second]
    flags = jnp.stack([core, half, my_quad, my_row]).astype(jnp.int32)
    hi, mid = prepare(flags, rows, parts, near_rows + second, theirs)
    wide = (group, 2 * piece_len)

    def sent_shape(step):
        return (2 * (quads - 2 - step) + 1, *wide)

    start, same, sent = call(
        first_kernel,
        flags,
        (incoming.reshape(rows, QUAD, group, piece_len), hi, mid),
        (wide, wide, sent_shape(0)),
    )
    final = start
    for step in range(quads - 1):
        far_to = pairs(lambda q, i: (next_quad(q, step, quads), i))
        near_to = pairs(lambda q, i: (next_quad(q, step, quads), i ^ 2))
        far = lax.ppermute(same, ("quad", "i"), far_to)
        got = lax.ppermute(sent, ("quad", "i"), near_to)
        args, outs = (start, got, far, final), (wide,)
        if step + 2 < quads:
            args, outs = (*args, hi, mid), (wide, wide, sent_shape(step + 1))
        final, *rest = call(functools.partial(step_kernel, step + 1), flags, args, outs)
        if rest:
            same, sent = rest
    final = jnp.where(core == 0, final[:, :piece_len], final[:, piece_len:])
    whole = lax.all_to_all(
        jnp.broadcast_to(final[None], (rows, group, piece_len)), "row", 0, 0, tiled=True
    )
    return whole.reshape(rhs_count, 1, 1, piece_len)


def solution(mesh):
    rows, cols = mesh.devices.shape
    grid = Mesh(mesh.devices.reshape(rows, cols // QUAD, QUAD), ("row", "quad", "i"))
    return jax.shard_map(
        solve,
        mesh=grid,
        in_specs=(
            P(None, ("row", "quad", "i")),
            P(),
            P("row", None, ("quad", "i"), None),
            P("row", None, None),
        ),
        out_specs=P(None, None, ("quad", "i"), None),
        check_vma=False,
    )
```

```python
import functools

import jax
import jax.numpy as jnp
from jax import lax
from jax.experimental import pallas as pl
from jax.experimental.pallas import tpu as pltpu
from jax.sharding import Mesh
from jax.sharding import PartitionSpec as P


QUAD = 4
VMEM_LIMIT = 16 * 2**20


def dot(a, b, contract):
    return lax.dot_general(
        a,
        b,
        (contract, ((), ())),
        precision=lax.Precision.HIGHEST,
        preferred_element_type=jnp.float32,
    )


def split3(x):
    hi = x.astype(jnp.bfloat16)
    rest = x - hi.astype(jnp.float32)
    mid = rest.astype(jnp.bfloat16)
    lo = (rest - mid.astype(jnp.float32)).astype(jnp.bfloat16)
    return hi, mid, lo


def take_kernel(first_ref, pivots_ref, rhs_ref, out_ref):
    count, source = rhs_ref.shape
    located = pivots_ref[...] - first_ref[0]
    place = lax.broadcasted_iota(jnp.int32, (source, located.shape[1]), 0)
    pick = jnp.where(place == located, 1.0, 0.0).astype(jnp.bfloat16)
    parts = jnp.concatenate(split3(rhs_ref[...]), axis=0)
    got = jnp.dot(parts, pick, preferred_element_type=jnp.float32)
    got = (got[2 * count :] + got[count : 2 * count]) + got[:count]
    pieces, _, length = out_ref.shape
    for n in range(pieces):
        out_ref[n] = got[:, n * length : (n + 1) * length]


def take_columns(rhs, pivots, first, piece_len):
    count, source = rhs.shape
    total = pivots.shape[0]
    step = source
    return pl.pallas_call(
        take_kernel,
        grid=(total // step,),
        in_specs=[
            pl.BlockSpec(memory_space=pltpu.SMEM),
            pl.BlockSpec((1, step), lambda n: (0, n)),
            pl.BlockSpec((count, source), lambda n: (0, 0)),
        ],
        out_specs=pl.BlockSpec((step // piece_len, count, piece_len), lambda n: (n, 0, 0)),
        out_shape=jax.ShapeDtypeStruct((total // piece_len, count, piece_len), jnp.float32),
        compiler_params=pltpu.CompilerParams(vmem_limit_bytes=VMEM_LIMIT),
    )(first.reshape(1), pivots.reshape(1, total), rhs)


def split2(x):
    hi = x.astype(jnp.bfloat16)
    return hi, (x - hi.astype(jnp.float32)).astype(jnp.bfloat16)


NN = ((1,), (0,))
NT = ((1,), (1,))


def product(y, hi, mid, contract):
    rows = y.shape[0]
    y_hi, y_mid = split2(y)

    def mul(a, b):
        return lax.dot_general(a, b, (contract, ((), ())), preferred_element_type=jnp.float32)

    wide = mul(jnp.concatenate([y_hi, y_mid], axis=0), hi)
    return wide[:rows] + (wide[rows:] + mul(y_hi, mid))


def prep_kernel(parts, flags_ref, *refs):
    count = len(parts)
    mine, theirs = refs[:count], refs[count : 2 * count]
    hi_ref, mid_ref = refs[-2:]
    rows = hi_ref.shape[0]
    length = mine[0].shape[0]
    core = flags_ref[0]

    def put(row, place, offset, value):
        start = pl.multiple_of(place * length + offset, value.shape[0])
        at = pl.ds(start, value.shape[0])
        hi_ref[row, at, :], mid_ref[row, at, :] = split2(value)

    for n, (distance, offset) in enumerate(parts):
        row = lax.rem(flags_ref[3] + (distance + rows), rows)
        put(row, core, offset, mine[n][...])
        put(row, 1 - core, offset, theirs[n][...])


def prepare(flags, rows, parts, mine, theirs):
    length, width = mine[0].shape
    shape = (rows, 2 * length, width)
    vmem = pl.BlockSpec(memory_space=pltpu.VMEM)
    return pl.pallas_call(
        functools.partial(prep_kernel, parts),
        in_specs=[pl.BlockSpec(memory_space=pltpu.SMEM)] + [vmem] * (len(mine) + len(theirs)),
        out_specs=[vmem, vmem],
        out_shape=[pltpu.VMEM(shape, jnp.bfloat16)] * 2,
        compiler_params=pltpu.CompilerParams(vmem_limit_bytes=VMEM_LIMIT),
    )(flags, *mine, *theirs)


def contributions(step, flags_ref, y, earlier, hi_ref, mid_ref, same_ref, sent_ref):
    half_len = y.shape[1]
    for n in range(step + 1, hi_ref.shape[0]):
        got = product(y, hi_ref[n], mid_ref[n], NN)
        low, high = got[:, :half_len], got[:, half_len:]
        k = n - step - 1
        if earlier is not None:
            low = low + earlier[1 + 2 * k]
            high = high + earlier[2 + 2 * k]
        if k == 0:
            same_ref[...] = jnp.where(flags_ref[1] == 0, low, high)
            sent_ref[0] = jnp.where(flags_ref[1] == 0, high, low)
        else:
            sent_ref[2 * k - 1] = low
            sent_ref[2 * k] = high


def first_kernel(flags_ref, pieces_ref, hi_ref, mid_ref, start_ref, same_ref, sent_ref):
    sums = jnp.sum(pieces_ref[...], axis=0)
    sums = jnp.where(flags_ref[4] == 1, jnp.concatenate([sums[2:], sums[:2]], axis=0), sums)
    block = jnp.concatenate([sums[i] for i in range(QUAD)], axis=1)
    own = flags_ref[2]
    start = product(block, hi_ref[own], mid_ref[own], NT)
    start_ref[...] = start
    contributions(0, flags_ref, start, None, hi_ref, mid_ref, same_ref, sent_ref)


def step_kernel(step, flags_ref, start_ref, near_ref, far_ref, final_ref, *rest):
    both = start_ref[...] + near_ref[0] + far_ref[...]
    kept = jnp.where(flags_ref[2] == step, both, final_ref[...])
    if len(rest) == 1:
        rest[0][...] = kept
        return
    hi_ref, mid_ref, kept_ref, same_ref, sent_ref = rest
    kept_ref[...] = kept
    contributions(step, flags_ref, both, near_ref, hi_ref, mid_ref, same_ref, sent_ref)


def call(kernel, flags, args, outs):
    vmem = pl.BlockSpec(memory_space=pltpu.VMEM)
    return pl.pallas_call(
        kernel,
        in_specs=[pl.BlockSpec(memory_space=pltpu.SMEM)] + [vmem] * len(args),
        out_specs=[vmem] * len(outs),
        out_shape=[jax.ShapeDtypeStruct(shape, jnp.float32) for shape in outs],
        compiler_params=pltpu.CompilerParams(vmem_limit_bytes=VMEM_LIMIT),
    )(flags, *args)


def mirrored(quad, i):
    if quad // 2 % 2:
        return quad, i
    return quad ^ 1, i ^ 2


def next_quad(quad, step, quads):
    if step % 2 == 0:
        return quad ^ 1
    turn, side = quad // 2, quad % 2
    turn = turn ^ 1 if step % 4 == 1 else (turn + 1 if turn % 2 else turn - 1) % (quads // 2)
    return 2 * turn + side


def solve(rhs, pivots, factor, diag_inv):
    my_row = lax.axis_index("row")
    my_quad = lax.axis_index("quad")
    my_i = lax.axis_index("i")
    rows = lax.axis_size("row")
    quads = lax.axis_size("quad")
    turned = my_quad // 2 % 2 == 0
    at_quad = jnp.where(turned, my_quad ^ 1, my_quad)
    at_i = jnp.where(turned, my_i ^ 2, my_i)
    core = at_i % 2
    half = at_i // 2
    rhs_count, source_len = rhs.shape
    block_len, _, _, piece_len = factor.shape
    group = rhs_count // rows
    flat = (my_row * quads + my_quad) * QUAD + my_i
    places = [(q, i) for q in range(quads) for i in range(QUAD)]

    def pairs(move):
        return [(q * QUAD + i, move(q, i)[0] * QUAD + move(q, i)[1]) for q, i in places]

    def mirror(shard):
        there = [(a, b) for a, b in pairs(mirrored) if a != b]
        return jnp.where(turned, lax.ppermute(shard, ("quad", "i"), there), shard)

    lower = mirror(factor.reshape(block_len, piece_len))
    order = pivots.reshape(quads // 2, 4, -1)
    even = lax.broadcasted_iota(jnp.int32, order.shape, 0) % 2 == 0
    order = jnp.where(even, order[:, ::-1], order).reshape(-1)
    taken = take_columns(rhs, order, flat * source_len, piece_len)
    inverse = diag_inv[0]
    scaled = dot(lower, inverse, ((0,), (1,)))
    own_rows = lax.dynamic_slice_in_dim(inverse, at_i * piece_len, piece_len, 0)
    slot = jnp.where(at_quad == my_row, own_rows, -scaled)

    def shift(shard, by):
        return lax.ppermute(shard, "row", [(r, (r + by) % rows) for r in range(rows)])

    partner = [(i, i ^ 1) for i in range(QUAD)]
    first = [shift(slot, 2), shift(slot, -2)]
    first += [shift(slot, 1), shift(slot, -1)]
    spread = lax.all_to_all(taken, ("quad", "i"), 0, 0, tiled=True)
    piece = spread.sum(axis=0)
    cut = piece_len // 2
    second = [
        shift(first[0][:cut], 2),
        shift(first[1][cut:], -2),
        shift(first[0], 1),
        shift(first[1], -1),
    ]
    parts = ((0, 0), (-2, 0), (2, 0), (-1, 0), (1, 0), (4, 0), (4, cut), (-3, 0), (3, 0))
    near_rows = [slot, *first]
    theirs = [lax.ppermute(rows_of, "i", partner) for rows_of in near_rows]
    outgoing = jnp.broadcast_to(
        piece.reshape(rows, 1, group, piece_len), (rows, QUAD, group, piece_len)
    ).reshape(rows * QUAD, group, piece_len)
    incoming = lax.all_to_all(outgoing, ("row", "i"), 0, 0, tiled=True)
    incoming, *second = lax.optimization_barrier((incoming, *second))
    theirs += [lax.ppermute(rows_of, "i", partner) for rows_of in second]
    flags = jnp.stack([core, half, at_quad, my_row, turned.astype(jnp.int32)]).astype(jnp.int32)
    hi, mid = prepare(flags, rows, parts, near_rows + second, theirs)
    wide = (group, 2 * piece_len)

    def sent_shape(step):
        return (2 * (quads - 2 - step) + 1, *wide)

    start, same, sent = call(
        first_kernel,
        flags,
        (incoming.reshape(rows, QUAD, group, piece_len), hi, mid),
        (wide, wide, sent_shape(0)),
    )
    final = start
    for step in range(quads - 1):
        near = 2 if step % 2 == 0 else 0
        far_to = pairs(lambda q, i: (next_quad(q, step, quads), i ^ 2 ^ near))
        near_to = pairs(lambda q, i: (next_quad(q, step, quads), i ^ near))
        far = lax.ppermute(same, ("quad", "i"), far_to)
        got = lax.ppermute(sent, ("quad", "i"), near_to)
        args, outs = (start, got, far, final), (wide,)
        if step + 2 < quads:
            args, outs = (*args, hi, mid), (wide, wide, sent_shape(step + 1))
        final, *rest = call(functools.partial(step_kernel, step + 1), flags, args, outs)
        if rest:
            same, sent = rest
        if step == quads - 4:
            home = mirror(final)
    final = jnp.where(turned, home, final)
    final = jnp.where(core == 0, final[:, :piece_len], final[:, piece_len:])
    whole = lax.all_to_all(
        jnp.broadcast_to(final[None], (rows, group, piece_len)), "row", 0, 0, tiled=True
    )
    return whole.reshape(rhs_count, 1, 1, piece_len)


def solution(mesh):
    rows, cols = mesh.devices.shape
    grid = Mesh(mesh.devices.reshape(rows, cols // QUAD, QUAD), ("row", "quad", "i"))
    return jax.shard_map(
        solve,
        mesh=grid,
        in_specs=(
            P(None, ("row", "quad", "i")),
            P(),
            P("row", None, ("quad", "i"), None),
            P("row", None, None),
        ),
        out_specs=P(None, None, ("quad", "i"), None),
        check_vma=False,
    )
```

```python
import functools

import jax
import jax.numpy as jnp
from jax import lax
from jax.experimental import pallas as pl
from jax.experimental.pallas import tpu as pltpu
from jax.sharding import Mesh
from jax.sharding import PartitionSpec as P


QUAD = 4
VMEM_LIMIT = 16 * 2**20


def dot(a, b, contract):
    return lax.dot_general(
        a,
        b,
        (contract, ((), ())),
        precision=lax.Precision.HIGHEST,
        preferred_element_type=jnp.float32,
    )


def split3(x):
    hi = x.astype(jnp.bfloat16)
    rest = x - hi.astype(jnp.float32)
    mid = rest.astype(jnp.bfloat16)
    lo = (rest - mid.astype(jnp.float32)).astype(jnp.bfloat16)
    return hi, mid, lo


def turned_quad(quad):
    return 1 - ((quad >> 1) & 1)


def take_kernel(first_ref, pivots_ref, rhs_ref, out_ref):
    count, source = rhs_ref.shape
    located = pivots_ref[...] - first_ref[0]
    place = lax.broadcasted_iota(jnp.int32, (source, located.shape[1]), 0)
    pick = jnp.where(place == located, 1.0, 0.0).astype(jnp.bfloat16)
    parts = jnp.concatenate(split3(rhs_ref[...]), axis=0)
    got = jnp.dot(parts, pick, preferred_element_type=jnp.float32)
    got = (got[2 * count :] + got[count : 2 * count]) + got[:count]
    pieces, _, length = out_ref.shape
    shift = 2 * turned_quad(pl.program_id(0))
    for n in range(pieces):
        out_ref[lax.rem(n + shift, pieces)] = got[:, n * length : (n + 1) * length]


def take_columns(rhs, pivots, first, piece_len):
    count, source = rhs.shape
    total = pivots.shape[0]
    step = QUAD * piece_len
    return pl.pallas_call(
        take_kernel,
        grid=(total // step,),
        in_specs=[
            pl.BlockSpec(memory_space=pltpu.SMEM),
            pl.BlockSpec((1, step), lambda n: (0, n)),
            pl.BlockSpec((count, source), lambda n: (0, 0)),
        ],
        out_specs=pl.BlockSpec(
            (step // piece_len, count, piece_len), lambda n: (n ^ turned_quad(n), 0, 0)
        ),
        out_shape=jax.ShapeDtypeStruct((total // piece_len, count, piece_len), jnp.float32),
        compiler_params=pltpu.CompilerParams(vmem_limit_bytes=VMEM_LIMIT),
    )(first.reshape(1), pivots.reshape(1, total), rhs)


def split2(x):
    hi = x.astype(jnp.bfloat16)
    return hi, (x - hi.astype(jnp.float32)).astype(jnp.bfloat16)


NN = ((1,), (0,))
NT = ((1,), (1,))


def product(y, hi, mid, contract):
    rows = y.shape[0]
    y_hi, y_mid = split2(y)

    def mul(a, b):
        return lax.dot_general(a, b, (contract, ((), ())), preferred_element_type=jnp.float32)

    wide = mul(jnp.concatenate([y_hi, y_mid], axis=0), hi)
    return wide[:rows] + (wide[rows:] + mul(y_hi, mid))


def prep_kernel(parts, flags_ref, *refs):
    count = len(parts)
    mine, theirs = refs[:count], refs[count : 2 * count]
    hi_ref, mid_ref = refs[-2:]
    rows = hi_ref.shape[0]
    length = mine[0].shape[0]
    core = flags_ref[0]

    def put(row, place, offset, value):
        start = pl.multiple_of(place * length + offset, value.shape[0])
        at = pl.ds(start, value.shape[0])
        hi_ref[row, at, :], mid_ref[row, at, :] = split2(value)

    for n, (distance, offset) in enumerate(parts):
        row = lax.rem(flags_ref[3] + (distance + rows), rows)
        put(row, core, offset, mine[n][...])
        put(row, 1 - core, offset, theirs[n][...])


def prepare(flags, rows, parts, mine, theirs):
    length, width = mine[0].shape
    shape = (rows, 2 * length, width)
    vmem = pl.BlockSpec(memory_space=pltpu.VMEM)
    return pl.pallas_call(
        functools.partial(prep_kernel, parts),
        in_specs=[pl.BlockSpec(memory_space=pltpu.SMEM)] + [vmem] * (len(mine) + len(theirs)),
        out_specs=[vmem, vmem],
        out_shape=[pltpu.VMEM(shape, jnp.bfloat16)] * 2,
        compiler_params=pltpu.CompilerParams(vmem_limit_bytes=VMEM_LIMIT),
    )(flags, *mine, *theirs)


def contributions(step, flags_ref, y, earlier, hi_ref, mid_ref, same_ref, sent_ref):
    half_len = y.shape[1]
    for n in range(step + 1, hi_ref.shape[0]):
        got = product(y, hi_ref[n], mid_ref[n], NN)
        low, high = got[:, :half_len], got[:, half_len:]
        k = n - step - 1
        if earlier is not None:
            low = low + earlier[1 + 2 * k]
            high = high + earlier[2 + 2 * k]
        if k == 0:
            same_ref[...] = jnp.where(flags_ref[1] == 0, low, high)
            sent_ref[0] = jnp.where(flags_ref[1] == 0, high, low)
        else:
            sent_ref[2 * k - 1] = low
            sent_ref[2 * k] = high


def first_kernel(flags_ref, pieces_ref, hi_ref, mid_ref, start_ref, same_ref, sent_ref):
    sums = jnp.sum(pieces_ref[...], axis=0)
    sums = jnp.where(flags_ref[4] == 1, jnp.concatenate([sums[2:], sums[:2]], axis=0), sums)
    block = jnp.concatenate([sums[i] for i in range(QUAD)], axis=1)
    own = flags_ref[2]
    start = product(block, hi_ref[own], mid_ref[own], NT)
    start_ref[...] = start
    contributions(0, flags_ref, start, None, hi_ref, mid_ref, same_ref, sent_ref)


def step_kernel(step, flags_ref, start_ref, near_ref, far_ref, final_ref, *rest):
    both = start_ref[...] + near_ref[0] + far_ref[...]
    kept = jnp.where(flags_ref[2] == step, both, final_ref[...])
    if len(rest) == 1:
        rest[0][...] = kept
        return
    hi_ref, mid_ref, kept_ref, same_ref, sent_ref = rest
    kept_ref[...] = kept
    contributions(step, flags_ref, both, near_ref, hi_ref, mid_ref, same_ref, sent_ref)


def call(kernel, flags, args, outs):
    vmem = pl.BlockSpec(memory_space=pltpu.VMEM)
    return pl.pallas_call(
        kernel,
        in_specs=[pl.BlockSpec(memory_space=pltpu.SMEM)] + [vmem] * len(args),
        out_specs=[vmem] * len(outs),
        out_shape=[jax.ShapeDtypeStruct(shape, jnp.float32) for shape in outs],
        compiler_params=pltpu.CompilerParams(vmem_limit_bytes=VMEM_LIMIT),
    )(flags, *args)


def mirrored(quad, i):
    if quad // 2 % 2:
        return quad, i
    return quad ^ 1, i ^ 2


def next_quad(quad, step, quads):
    if step % 2 == 0:
        return quad ^ 1
    turn, side = quad // 2, quad % 2
    turn = turn ^ 1 if step % 4 == 1 else (turn + 1 if turn % 2 else turn - 1) % (quads // 2)
    return 2 * turn + side


def solve(rhs, pivots, factor, diag_inv):
    my_row = lax.axis_index("row")
    my_quad = lax.axis_index("quad")
    my_i = lax.axis_index("i")
    rows = lax.axis_size("row")
    quads = lax.axis_size("quad")
    turned = my_quad // 2 % 2 == 0
    at_quad = jnp.where(turned, my_quad ^ 1, my_quad)
    at_i = jnp.where(turned, my_i ^ 2, my_i)
    core = at_i % 2
    half = at_i // 2
    rhs_count, source_len = rhs.shape
    block_len, _, _, piece_len = factor.shape
    group = rhs_count // rows
    flat = (my_row * quads + my_quad) * QUAD + my_i
    places = [(q, i) for q in range(quads) for i in range(QUAD)]

    def pairs(move):
        return [(q * QUAD + i, move(q, i)[0] * QUAD + move(q, i)[1]) for q, i in places]

    def mirror(shard):
        there = [(a, b) for a, b in pairs(mirrored) if a != b]
        return jnp.where(turned, lax.ppermute(shard, ("quad", "i"), there), shard)

    lower = mirror(factor.reshape(block_len, piece_len))
    taken = take_columns(rhs, pivots, flat * source_len, piece_len)
    inverse = diag_inv[0]
    scaled = dot(lower, inverse, ((0,), (1,)))
    own_rows = lax.dynamic_slice_in_dim(inverse, at_i * piece_len, piece_len, 0)
    slot = jnp.where(at_quad == my_row, own_rows, -scaled)

    def shift(shard, by):
        return lax.ppermute(shard, "row", [(r, (r + by) % rows) for r in range(rows)])

    partner = [(i, i ^ 1) for i in range(QUAD)]
    first = [shift(slot, 2), shift(slot, -2)]
    first += [shift(slot, 1), shift(slot, -1)]
    spread = lax.all_to_all(taken, ("quad", "i"), 0, 0, tiled=True)
    piece = spread.sum(axis=0)
    cut = piece_len // 2
    second = [
        shift(first[0][:cut], 2),
        shift(first[1][cut:], -2),
        shift(first[0], 1),
        shift(first[1], -1),
    ]
    parts = ((0, 0), (-2, 0), (2, 0), (-1, 0), (1, 0), (4, 0), (4, cut), (-3, 0), (3, 0))
    near_rows = [slot, *first]
    theirs = [lax.ppermute(rows_of, "i", partner) for rows_of in near_rows]
    outgoing = jnp.broadcast_to(
        piece.reshape(rows, 1, group, piece_len), (rows, QUAD, group, piece_len)
    ).reshape(rows * QUAD, group, piece_len)
    incoming = lax.all_to_all(outgoing, ("row", "i"), 0, 0, tiled=True)
    incoming, *second = lax.optimization_barrier((incoming, *second))
    theirs += [lax.ppermute(rows_of, "i", partner) for rows_of in second]
    flags = jnp.stack([core, half, at_quad, my_row, turned.astype(jnp.int32)]).astype(jnp.int32)
    hi, mid = prepare(flags, rows, parts, near_rows + second, theirs)
    wide = (group, 2 * piece_len)

    def sent_shape(step):
        return (2 * (quads - 2 - step) + 1, *wide)

    start, same, sent = call(
        first_kernel,
        flags,
        (incoming.reshape(rows, QUAD, group, piece_len), hi, mid),
        (wide, wide, sent_shape(0)),
    )
    final = start
    for step in range(quads - 1):
        near = 2 if step % 2 == 0 else 0
        far_to = pairs(lambda q, i: (next_quad(q, step, quads), i ^ 2 ^ near))
        near_to = pairs(lambda q, i: (next_quad(q, step, quads), i ^ near))
        far = lax.ppermute(same, ("quad", "i"), far_to)
        got = lax.ppermute(sent, ("quad", "i"), near_to)
        args, outs = (start, got, far, final), (wide,)
        if step + 2 < quads:
            args, outs = (*args, hi, mid), (wide, wide, sent_shape(step + 1))
        final, *rest = call(functools.partial(step_kernel, step + 1), flags, args, outs)
        if rest:
            same, sent = rest
        if step == quads - 4:
            home = mirror(final)
    final = jnp.where(turned, home, final)
    final = jnp.where(core == 0, final[:, :piece_len], final[:, piece_len:])
    whole = lax.all_to_all(
        jnp.broadcast_to(final[None], (rows, group, piece_len)), "row", 0, 0, tiled=True
    )
    return whole.reshape(rhs_count, 1, 1, piece_len)


def solution(mesh):
    rows, cols = mesh.devices.shape
    grid = Mesh(mesh.devices.reshape(rows, cols // QUAD, QUAD), ("row", "quad", "i"))
    return jax.shard_map(
        solve,
        mesh=grid,
        in_specs=(
            P(None, ("row", "quad", "i")),
            P(),
            P("row", None, ("quad", "i"), None),
            P("row", None, None),
        ),
        out_specs=P(None, None, ("quad", "i"), None),
        check_vma=False,
    )
```

```python
import functools

import jax
import jax.numpy as jnp
from jax import lax
from jax.experimental import pallas as pl
from jax.experimental.pallas import tpu as pltpu
from jax.sharding import Mesh
from jax.sharding import PartitionSpec as P


QUAD = 4
VMEM_LIMIT = 16 * 2**20


def dot(a, b, contract):
    return lax.dot_general(
        a,
        b,
        (contract, ((), ())),
        precision=lax.Precision.HIGHEST,
        preferred_element_type=jnp.float32,
    )


def split3(x):
    hi = x.astype(jnp.bfloat16)
    rest = x - hi.astype(jnp.float32)
    mid = rest.astype(jnp.bfloat16)
    lo = (rest - mid.astype(jnp.float32)).astype(jnp.bfloat16)
    return hi, mid, lo


def turned_quad(quad):
    return 1 - ((quad >> 1) & 1)


def take_kernel(first_ref, pivots_ref, rhs_ref, out_ref):
    count, source = rhs_ref.shape
    located = pivots_ref[...] - first_ref[0]
    place = lax.broadcasted_iota(jnp.int32, (source, located.shape[1]), 0)
    pick = jnp.where(place == located, 1.0, 0.0).astype(jnp.bfloat16)
    parts = jnp.concatenate(split3(rhs_ref[...]), axis=0)
    got = jnp.dot(parts, pick, preferred_element_type=jnp.float32)
    got = (got[2 * count :] + got[count : 2 * count]) + got[:count]
    pieces, _, length = out_ref.shape
    shift = 2 * turned_quad(pl.program_id(0))
    for n in range(pieces):
        out_ref[lax.rem(n + shift, pieces)] = got[:, n * length : (n + 1) * length]


def take_columns(rhs, pivots, first, piece_len):
    count, source = rhs.shape
    total = pivots.shape[0]
    step = QUAD * piece_len
    return pl.pallas_call(
        take_kernel,
        grid=(total // step,),
        in_specs=[
            pl.BlockSpec(memory_space=pltpu.SMEM),
            pl.BlockSpec((1, step), lambda n: (0, n)),
            pl.BlockSpec((count, source), lambda n: (0, 0)),
        ],
        out_specs=pl.BlockSpec(
            (step // piece_len, count, piece_len), lambda n: (n ^ turned_quad(n), 0, 0)
        ),
        out_shape=jax.ShapeDtypeStruct((total // piece_len, count, piece_len), jnp.float32),
        compiler_params=pltpu.CompilerParams(vmem_limit_bytes=VMEM_LIMIT),
    )(first.reshape(1), pivots.reshape(1, total), rhs)


def split2(x):
    hi = x.astype(jnp.bfloat16)
    return hi, (x - hi.astype(jnp.float32)).astype(jnp.bfloat16)


NN = ((1,), (0,))
NT = ((1,), (1,))


def product(y, hi, mid, contract):
    rows = y.shape[0]
    y_hi, y_mid = split2(y)

    def mul(a, b):
        return lax.dot_general(a, b, (contract, ((), ())), preferred_element_type=jnp.float32)

    wide = mul(jnp.concatenate([y_hi, y_mid], axis=0), hi)
    return wide[:rows] + (wide[rows:] + mul(y_hi, mid))


def prep_kernel(parts, flags_ref, *refs):
    count = len(parts)
    mine, theirs = refs[:count], refs[count : 2 * count]
    hi_ref, mid_ref = refs[-2:]
    rows = hi_ref.shape[0]
    length = mine[0].shape[0]
    core = flags_ref[0]

    def put(row, place, offset, value):
        start = pl.multiple_of(place * length + offset, value.shape[0])
        at = pl.ds(start, value.shape[0])
        hi_ref[row, at, :], mid_ref[row, at, :] = split2(value)

    for n, (distance, offset) in enumerate(parts):
        row = lax.rem(flags_ref[3] + (distance + rows), rows)
        put(row, core, offset, mine[n][...])
        put(row, 1 - core, offset, theirs[n][...])


def prepare(flags, rows, parts, mine, theirs):
    length, width = mine[0].shape
    shape = (rows, 2 * length, width)
    vmem = pl.BlockSpec(memory_space=pltpu.VMEM)
    return pl.pallas_call(
        functools.partial(prep_kernel, parts),
        in_specs=[pl.BlockSpec(memory_space=pltpu.SMEM)] + [vmem] * (len(mine) + len(theirs)),
        out_specs=[vmem, vmem],
        out_shape=[pltpu.VMEM(shape, jnp.bfloat16)] * 2,
        compiler_params=pltpu.CompilerParams(vmem_limit_bytes=VMEM_LIMIT),
    )(flags, *mine, *theirs)


def contributions(step, flags_ref, y, earlier, hi_ref, mid_ref, same_ref, sent_ref):
    half_len = y.shape[1]
    for n in range(step + 1, hi_ref.shape[0]):
        got = product(y, hi_ref[n], mid_ref[n], NN)
        low, high = got[:, :half_len], got[:, half_len:]
        k = n - step - 1
        if earlier is not None:
            low = low + earlier[1 + 2 * k]
            high = high + earlier[2 + 2 * k]
        if k == 0:
            same_ref[...] = jnp.where(flags_ref[1] == 0, low, high)
            sent_ref[0] = jnp.where(flags_ref[1] == 0, high, low)
        else:
            sent_ref[2 * k - 1] = low
            sent_ref[2 * k] = high


def first_kernel(flags_ref, pieces_ref, hi_ref, mid_ref, start_ref, same_ref, sent_ref):
    sums = jnp.sum(pieces_ref[...], axis=0)
    sums = jnp.where(flags_ref[4] == 1, jnp.concatenate([sums[2:], sums[:2]], axis=0), sums)
    block = jnp.concatenate([sums[i] for i in range(QUAD)], axis=1)
    own = flags_ref[2]
    start = product(block, hi_ref[own], mid_ref[own], NT)
    start_ref[...] = start
    contributions(0, flags_ref, start, None, hi_ref, mid_ref, same_ref, sent_ref)


def step_kernel(step, flags_ref, start_ref, near_ref, far_ref, final_ref, *rest):
    both = start_ref[...] + near_ref[0] + far_ref[...]
    kept = jnp.where(flags_ref[2] == step, both, final_ref[...])
    if len(rest) == 1:
        rest[0][...] = kept
        return
    hi_ref, mid_ref, kept_ref, same_ref, sent_ref = rest
    kept_ref[...] = kept
    contributions(step, flags_ref, both, near_ref, hi_ref, mid_ref, same_ref, sent_ref)


def call(kernel, flags, args, outs):
    vmem = pl.BlockSpec(memory_space=pltpu.VMEM)
    return pl.pallas_call(
        kernel,
        in_specs=[pl.BlockSpec(memory_space=pltpu.SMEM)] + [vmem] * len(args),
        out_specs=[vmem] * len(outs),
        out_shape=[jax.ShapeDtypeStruct(shape, jnp.float32) for shape in outs],
        compiler_params=pltpu.CompilerParams(vmem_limit_bytes=VMEM_LIMIT),
    )(flags, *args)


def mirrored(quad, i):
    if quad // 2 % 2:
        return quad, i
    return quad ^ 1, i ^ 2


def next_quad(quad, step, quads):
    if step % 2 == 0:
        return quad ^ 1
    turn, side = quad // 2, quad % 2
    turn = turn ^ 1 if step % 4 == 1 else (turn + 1 if turn % 2 else turn - 1) % (quads // 2)
    return 2 * turn + side


def solve(rhs, pivots, factor, diag_inv):
    my_row = lax.axis_index("row")
    my_quad = lax.axis_index("quad")
    my_i = lax.axis_index("i")
    rows = lax.axis_size("row")
    quads = lax.axis_size("quad")
    turned = my_quad // 2 % 2 == 0
    at_quad = jnp.where(turned, my_quad ^ 1, my_quad)
    at_i = jnp.where(turned, my_i ^ 2, my_i)
    core = at_i % 2
    half = at_i // 2
    rhs_count, source_len = rhs.shape
    block_len, _, _, piece_len = factor.shape
    group = rhs_count // rows
    flat = (my_row * quads + my_quad) * QUAD + my_i
    places = [(q, i) for q in range(quads) for i in range(QUAD)]

    def pairs(move):
        return [(q * QUAD + i, move(q, i)[0] * QUAD + move(q, i)[1]) for q, i in places]

    def mirror(shard):
        there = [(a, b) for a, b in pairs(mirrored) if a != b]
        return jnp.where(turned, lax.ppermute(shard, ("quad", "i"), there), shard)

    lower = mirror(factor.reshape(block_len, piece_len))
    taken = take_columns(rhs, pivots, flat * source_len, piece_len)
    inverse = diag_inv[0]
    scaled = dot(lower, inverse, ((0,), (1,)))
    own_rows = lax.dynamic_slice_in_dim(inverse, at_i * piece_len, piece_len, 0)
    slot = jnp.where(at_quad == my_row, own_rows, -scaled)

    def shift(shard, by):
        return lax.ppermute(shard, "row", [(r, (r + by) % rows) for r in range(rows)])

    partner = [(i, i ^ 1) for i in range(QUAD)]
    first = [shift(slot, 2), shift(slot, -2)]
    first += [shift(slot, 1), shift(slot, -1)]
    spread = lax.all_to_all(taken, ("quad", "i"), 0, 0, tiled=True)
    piece = spread.sum(axis=0)
    second = [shift(first[0], 2), shift(first[0], 1), shift(first[1], -1)]
    parts = ((0, 0), (-2, 0), (2, 0), (-1, 0), (1, 0), (-4, 0), (-3, 0), (3, 0))
    near_rows = [slot, *first]
    theirs = [lax.ppermute(rows_of, "i", partner) for rows_of in near_rows]
    outgoing = jnp.broadcast_to(
        piece.reshape(rows, 1, group, piece_len), (rows, QUAD, group, piece_len)
    ).reshape(rows * QUAD, group, piece_len)
    incoming = lax.all_to_all(outgoing, ("row", "i"), 0, 0, tiled=True)
    incoming, *second = lax.optimization_barrier((incoming, *second))
    theirs += [lax.ppermute(rows_of, "i", partner) for rows_of in second]
    flags = jnp.stack([core, half, at_quad, my_row, turned.astype(jnp.int32)]).astype(jnp.int32)
    hi, mid = prepare(flags, rows, parts, near_rows + second, theirs)
    wide = (group, 2 * piece_len)

    def sent_shape(step):
        return (2 * (quads - 2 - step) + 1, *wide)

    start, same, sent = call(
        first_kernel,
        flags,
        (incoming.reshape(rows, QUAD, group, piece_len), hi, mid),
        (wide, wide, sent_shape(0)),
    )
    final = start
    for step in range(quads - 1):
        near = 2 if step % 2 == 0 else 0
        far_to = pairs(lambda q, i: (next_quad(q, step, quads), i ^ 2 ^ near))
        near_to = pairs(lambda q, i: (next_quad(q, step, quads), i ^ near))
        far = lax.ppermute(same, ("quad", "i"), far_to)
        got = lax.ppermute(sent, ("quad", "i"), near_to)
        args, outs = (start, got, far, final), (wide,)
        if step + 2 < quads:
            args, outs = (*args, hi, mid), (wide, wide, sent_shape(step + 1))
        final, *rest = call(functools.partial(step_kernel, step + 1), flags, args, outs)
        if rest:
            same, sent = rest
        if step == quads - 4:
            home = mirror(final)
    final = jnp.where(turned, home, final)
    final = jnp.where(core == 0, final[:, :piece_len], final[:, piece_len:])
    whole = lax.all_to_all(
        jnp.broadcast_to(final[None], (rows, group, piece_len)), "row", 0, 0, tiled=True
    )
    return whole.reshape(rhs_count, 1, 1, piece_len)


def solution(mesh):
    rows, cols = mesh.devices.shape
    grid = Mesh(mesh.devices.reshape(rows, cols // QUAD, QUAD), ("row", "quad", "i"))
    return jax.shard_map(
        solve,
        mesh=grid,
        in_specs=(
            P(None, ("row", "quad", "i")),
            P(),
            P("row", None, ("quad", "i"), None),
            P("row", None, None),
        ),
        out_specs=P(None, None, ("quad", "i"), None),
        check_vma=False,
    )
```
